256 devices in a mesh: groups: 2 (over z), pre: 16 (over y, core), dec: 8 (over x).
Axes of the slice: x: 8, y: 8, z: 2, core: 2. Of those that a mesh axis runs over, the one named last changes fastest.
The devices are a block of a 8x8x16 slice.
Arguments:
- tokens: bfloat16 [32768, 2048], P(('groups', 'pre', 'dec')), parts along dimension 0, may hold values from -6 to 6
- attended: bfloat16 [32768, 2048], P(('groups', 'pre', 'dec')), parts along dimension 0, may hold values from -6 to 6
- input_gain: float32 [2048], replicated, may hold values from 0.25 to 1.75
- post_gain: float32 [2048], replicated, may hold values from 0.25 to 1.75
- kv_weight: bfloat16 [2048, 1024], P('pre'), may hold values from -0.125 to 0.125
- key_gain: float32 [128], replicated, may hold values from 0.25 to 1.75
- w_gate: bfloat16 [128, 2048, 768], P(('pre', 'dec')), may hold values from -0.125 to 0.125
- w_up: bfloat16 [128, 2048, 768], P(('pre', 'dec')), may hold values from -0.125 to 0.125
- w_down: bfloat16 [128, 768, 2048], P(('pre', 'dec')), may hold values from -0.21875 to 0.21875
- expert_ids: int32 [32768, 8], P(('groups', 'pre', 'dec')), parts along dimension 0, may hold values from 0 to 127, all different within a row; in each aligned block of 128 rows (0 to 127, 128 to 255, ...) at most 10 rows name the same one
- gate_weights: float32 [32768, 8], P(('groups', 'pre', 'dec')), parts along dimension 0, may hold values from 0.05 to 1
- page_list: int32 [32, 64], P(('groups', 'pre')), parts along dimension 0, may hold values from 0 to 63, each once within a row
- lengths: int32 [32, 8], P(('groups', 'pre')), parts along dimension 0, may hold values from 1 to 16, 64 in all within a row
- assignment: int32 [256, 1], P(('groups', 'pre')), parts along dimension 0, may hold values from 0 to 7; in each aligned block of 8 rows (0 to 7, 8 to 15, ...) at most 3 rows name the same one
- query: bfloat16 [256, 4096], P(('groups', 'pre')), parts along dimension 0, may hold values from -300 to 300
- new_kv: bfloat16 [256, 1024], P(('groups', 'pre')), parts along dimension 0, may hold values from -6 to 6
Outputs:
- moe_out: bfloat16 [32768, 2048], P(('groups', 'pre', 'dec')), parts along dimension 0
- decode_out: bfloat16 [768, 4096], P(('groups', 'pre', 'dec')), parts along dimension 0
The draws below stay inside these ranges and needn't reach their ends.
There are 2 independent parts, one for each index of `groups`. The reference program is written for one: setup_inputs(seed, part) draws one part's arguments, and reference() takes and returns one part's arrays. A program takes and returns all parts, laid end to end along the dimension named above; an argument that names none is the same for every part. Nothing has to cross between parts.
Inputs may be any that keep to these rules, and one draw needn't show every extreme that they name: `expert_ids`: each row names 8 different experts; among the rows of one device no expert is named by more than 10 rows, and some expert reaches 10. `page_list`: each slab's row names each of its pages once. Each slab's lengths sum to 64. `assignment`: within each aligned block of 8 requests (one slab) no decoding device is named more than 3 times, and some block reaches 3.
All inputs are finite; a program needn't handle non-finite values.
Results may differ from the reference program's by a relative error of at most 0.0055.
The reference program's roundings to bfloat16 on the way count: a program that leaves them out, or rounds other values in their place, can miss the bound.
Values may be sent and summed in bfloat16 or wider, within the bound.
A program may use at most 128 MiB of HBM per device.

```python
import math
import jax
import jax.numpy as jnp
import numpy as np
from jax import lax

D = 2048
FF = 768
H = 32
KVH = 4
HD = 128
TOP = 8
TOK_DEV = 128
PAGE = 16
RCAP = 3
EXPERTS = 128
TOKENS = 16384
CAP = 10
PAGES_ROW = 64
MAXP = 16
REQ_ROW = 8
REQUESTS = 128
SLOTS = 384
N_PRE = 16
N_DEC = 8


def draw_query(key, part):
    base = jax.random.normal(jax.random.fold_in(key, 11), (REQUESTS, H * HD), jnp.float32)
    return jnp.clip(base, -300.0, 300.0).astype(jnp.bfloat16)


def block_scale(key, extent, cuts, smallest, high):
    loudness, own = 1.0, jax.random.fold_in(key, 6)
    for axis_at, parts in cuts:
        heights = jnp.exp(jax.random.uniform(jax.random.fold_in(own, axis_at), (parts,), jnp.float32, smallest / len(cuts), high / len(cuts)))
        loudness = loudness * jnp.repeat(heights, extent[axis_at] // parts).reshape([-1 if axis == axis_at else 1 for axis in range(len(extent))])
    return loudness


def split_up(count, total, bound, lean):
    portions = [(1 << 20) // math.isqrt(grade ** lean) + 1 for grade in range(2, count + 1)]
    rest, counts = total - bound - (count - 1), [1] * (count - 1)
    while rest > 0:
        movable = [i for i in range(count - 1) if counts[i] < bound]
        pool, budget = sum([portions[i] for i in movable]), rest
        for i in movable:
            more = min(bound - counts[i], max(1, budget * portions[i] // pool), rest)
            counts[i] = counts[i] + more
            rest = rest - more
    return np.array([bound] + counts)


def ragged_sizes(stream_key, number_of, total, limit, skew):
    if number_of == 2:
        one = jax.random.randint(stream_key, (), max(1, total - limit), min(limit, total - 1) + 1)
        return jnp.stack([one, total - one])
    sizes = jnp.asarray(split_up(number_of, total, limit, skew), jnp.int32)
    pairs = (number_of - 1) // 2
    donor, sink = sizes[1:1 + 2 * pairs:2], sizes[2:2 + 2 * pairs:2]
    margin = jnp.minimum(donor - 1, limit - sink)
    shifted = jax.random.randint(jax.random.fold_in(stream_key, 1), (pairs,), 0, 1 << 20) % (margin + 1)
    sizes = sizes.at[1:1 + 2 * pairs:2].set(donor - shifted).at[2:2 + 2 * pairs:2].set(sink + shifted)
    return sizes[jax.random.permutation(jax.random.fold_in(stream_key, 2), number_of)]


def deal_out(rng, own, number, rows, number_of, top, most, skew):
    order = jax.random.permutation(rng, number_of)
    crowded, usual = load_shares(number_of, rows * top, most, skew, True), load_shares(number_of, rows * top, most, skew, False)
    places = jnp.arange(number_of)

    def named(tallies, rotation):
        used = int((tallies > 0).sum())
        fixed = max(1, used // 4)
        shifted = fixed + (places - fixed + rotation * (used - fixed)) % max(1, number_of - fixed)
        return jnp.zeros((number_of,), jnp.int32).at[order[jnp.where(places < fixed, places, shifted)]].set(jnp.asarray(tallies, jnp.int32))

    tallies = jnp.where(number % 4 == 0, named(crowded, number // 4), named(usual, number - number // 4 - 1))
    mixed = jax.random.permutation(jax.random.fold_in(own, 3), number_of)
    donor, sink = mixed[0:number_of // 2 * 2:2], mixed[1:number_of // 2 * 2:2]
    slack = jnp.minimum(tallies[donor] - 1, most - tallies[sink]) // 2
    slack = jnp.where((donor == order[0]) | (sink == order[0]) | (tallies[sink] == 0), 0, jnp.maximum(slack, 0))
    shifted = jax.random.randint(jax.random.fold_in(own, 4), (number_of // 2,), 0, 1 << 20) % (slack + 1)
    tallies = tallies.at[donor].add(-shifted).at[sink].add(shifted)
    items = jnp.searchsorted(jnp.cumsum(tallies), jnp.arange(rows * top), side="right").astype(jnp.int32)
    table = items.reshape(top, rows).T
    table = table[jax.random.permutation(jax.random.fold_in(own, 1), rows)]
    rotation = jax.random.randint(jax.random.fold_in(own, 2), (rows, 1), 0, top)
    return jnp.take_along_axis(table, (jnp.arange(top)[None, :] + rotation) % top, axis=1)


def load_shares(number_of, total, reach, slope, full):
    loads = [(1 << 20) // math.isqrt(rank ** slope) + 1 for rank in range(1, number_of + 1)]
    largest = reach if full else min(reach, max(-(-total // number_of), total * loads[0] // sum(loads)))
    least = 1 if total - largest >= number_of - 1 else 0
    counts, spare = [largest] + [least] * (number_of - 1), total - largest - least * (number_of - 1)
    while spare > 0:
        candidates = [i for i in range(1, number_of) if counts[i] < largest] or [i for i in range(1, number_of) if counts[i] < reach]
        pool, remaining = sum([loads[i] for i in candidates]), spare
        for i in candidates:
            addition = min(reach - counts[i], max(1, remaining * loads[i] // pool), spare)
            counts[i] = counts[i] + addition
            spare = spare - addition
    return np.array(counts)


def normal_values(rng, shape, width, limit, shards=(), kind=jnp.bfloat16):
    factor_of = block_scale(rng, shape, shards, -0.22, 0.18) if shards else 1.0
    values = jax.random.normal(rng, shape, jnp.float32) * width * factor_of
    return jnp.minimum(jnp.maximum(values, -limit), limit).astype(kind)


def setup_inputs(seed: int = 0, part: int = 0) -> dict:
    streams_of = jax.random.split(jax.random.key(seed), 17)
    part_keys = jax.random.split(jax.random.fold_in(streams_of[16], part), 17)
    tokens = normal_values(part_keys[0], (TOKENS, D), 1.0, 6.0, ((0, 128),))
    attended = normal_values(part_keys[1], (TOKENS, D), 1.0, 6.0, ((0, 128),))
    input_gain = jnp.clip(1.0 + 0.15 * jax.random.normal(streams_of[2], (D,), jnp.float32), 0.25, 1.75)
    post_gain = jnp.clip(1.0 + 0.15 * jax.random.normal(streams_of[3], (D,), jnp.float32), 0.25, 1.75)
    kv_weight = normal_values(streams_of[4], (D, 2 * KVH * HD), D ** -0.5, 0.125, ((0, 16),))
    key_gain = jnp.clip(1.0 + 0.15 * jax.random.normal(streams_of[5], (HD,), jnp.float32), 0.25, 1.75)
    w_gate = normal_values(streams_of[6], (EXPERTS, D, FF), D ** -0.5, 0.125, ((0, 128),))
    w_up = normal_values(streams_of[7], (EXPERTS, D, FF), D ** -0.5, 0.125, ((0, 128),))
    w_down = normal_values(streams_of[8], (EXPERTS, FF, D), FF ** -0.5, 0.21875, ((0, 128),))
    expert_ids_keys = jax.random.split(jax.random.fold_in(part_keys[9], 1), TOKENS // TOK_DEV)
    expert_ids_turns = jax.random.permutation(jax.random.fold_in(part_keys[9], 3), TOKENS // TOK_DEV)
    expert_ids = jax.vmap(lambda own, number: deal_out(jax.random.fold_in(part_keys[9], 2), own, number, TOK_DEV, EXPERTS, TOP, CAP, 2))(expert_ids_keys, expert_ids_turns).reshape((TOKENS, TOP))
    gate_weights = jnp.clip(jnp.exp(math.log(1.0) - 2.9957323 * jax.random.uniform(part_keys[10], (TOKENS, TOP), jnp.float32) ** block_scale(part_keys[10], (TOKENS, TOP), ((0, 128),), -0.2, 0.2)), 0.05, 1.0)
    page_list = jax.vmap(lambda own: jax.random.permutation(own, PAGES_ROW))(jax.random.split(part_keys[11], N_PRE)).reshape((N_PRE, PAGES_ROW)).astype(jnp.int32)
    lengths = jax.vmap(lambda own: ragged_sizes(own, REQ_ROW, PAGES_ROW, MAXP, 2))(jax.random.split(part_keys[12], N_PRE)).reshape((N_PRE, REQ_ROW)).astype(jnp.int32)
    assignment_keys = jax.random.split(jax.random.fold_in(part_keys[13], 1), REQUESTS // REQ_ROW)
    assignment_turns = jax.random.permutation(jax.random.fold_in(part_keys[13], 3), REQUESTS // REQ_ROW)
    assignment = jax.vmap(lambda own, number: deal_out(jax.random.fold_in(part_keys[13], 2), own, number, REQ_ROW, N_DEC, 1, RCAP, 2))(assignment_keys, assignment_turns).reshape((REQUESTS, 1))
    query = draw_query(jax.random.fold_in(jax.random.fold_in(streams_of[16], part), 71), part)
    new_kv = normal_values(part_keys[15], (REQUESTS, 2 * KVH * HD), 1.0, 6.0, ((0, 16),))
    return dict(tokens=tokens, attended=attended, input_gain=input_gain, post_gain=post_gain, kv_weight=kv_weight, key_gain=key_gain, w_gate=w_gate, w_up=w_up, w_down=w_down, expert_ids=expert_ids, gate_weights=gate_weights, page_list=page_list, lengths=lengths, assignment=assignment, query=query, new_kv=new_kv)


EPSILON = 1e-06
FLOOR_SCORE = -1e+30

def norm_rows(values, scales):
    values = values.astype(jnp.float32)
    factor = lax.rsqrt(lax.optimization_barrier(jnp.mean(values * values, axis=-1, keepdims=True)) + EPSILON)
    return values * factor * scales.astype(jnp.float32)

def token_requests(page_order, page_counts):
    page_total = page_order.shape[0]
    request_ends = jnp.cumsum(page_counts).astype(jnp.int32)
    positions = jnp.arange(page_total, dtype=jnp.int32)
    owner_at = lax.optimization_barrier(jnp.sum((positions[:, None] >= request_ends[None, :]).astype(jnp.int32), axis=1)).astype(jnp.int32)
    matches = page_order[:, None] == positions[None, :]
    page_owner = lax.optimization_barrier(jnp.sum(jnp.where(matches, owner_at[:, None], 0), axis=0)).astype(jnp.int32)
    return jnp.repeat(page_owner, PAGE)

def slot_requests(owners, device, slot_count):
    request_count = owners.shape[0]
    is_mine = (owners == device).astype(jnp.int32)
    order_mine = jnp.cumsum(is_mine).astype(jnp.int32) - 1
    slot_hit = (is_mine[None, :] == 1) & (order_mine[None, :] == jnp.arange(slot_count, dtype=jnp.int32)[:, None])
    targets = lax.optimization_barrier(jnp.sum(jnp.where(slot_hit, jnp.arange(request_count, dtype=jnp.int32)[None, :], 0), axis=1)).astype(jnp.int32)
    return (targets, jnp.any(slot_hit, axis=1))

def expert_slots(block_ids):
    flat_ids = block_ids.reshape(-1)
    picks = (flat_ids[:, None] == jnp.arange(EXPERTS, dtype=jnp.int32)[None, :]).astype(jnp.int32)
    before = lax.optimization_barrier(jnp.sum((jnp.cumsum(picks, axis=0).astype(jnp.int32) - 1) * picks, axis=1)).astype(jnp.int32)
    return (flat_ids * CAP + before).astype(jnp.int32)

def reference(tokens, attended, input_gain, post_gain, kv_weight, key_gain, w_gate, w_up, w_down, expert_ids, gate_weights, page_list, lengths, assignment, query, new_kv):
    blocks_all = N_PRE * N_DEC
    normed = norm_rows(attended, post_gain).astype(jnp.bfloat16).reshape(blocks_all, TOK_DEV, D)
    slot_index = jax.vmap(expert_slots)(expert_ids.reshape(blocks_all, TOK_DEV, TOP))
    source_rows = jnp.repeat(jnp.arange(TOK_DEV, dtype=jnp.int32), TOP)
    block_index = jnp.arange(blocks_all, dtype=jnp.int32)[:, None]
    table = jnp.full((blocks_all, EXPERTS * CAP), TOK_DEV, jnp.int32)
    table = table.at[block_index, slot_index].set(jnp.broadcast_to(source_rows[None, :], slot_index.shape))
    padded = jnp.concatenate([normed, jnp.zeros((blocks_all, 1, D), jnp.bfloat16)], axis=1)
    table = jnp.transpose(table.reshape(blocks_all, EXPERTS, CAP), (1, 0, 2))

    def expert_pass(inputs):
        row_index, gate_matrix, up_matrix, down_matrix = inputs
        chosen = padded[block_index, row_index].reshape(blocks_all * CAP, D)
        gate_part = jnp.dot(chosen, gate_matrix, preferred_element_type=jnp.float32)
        up_part = jnp.dot(chosen, up_matrix, preferred_element_type=jnp.float32)
        hidden = (jax.nn.silu(gate_part) * up_part).astype(jnp.bfloat16)
        result = jnp.dot(hidden, down_matrix, preferred_element_type=jnp.float32).astype(jnp.bfloat16)
        return result.reshape(blocks_all, CAP, D)
    expert_rows = lax.map(expert_pass, (table, w_gate, w_up, w_down))
    expert_rows = jnp.transpose(expert_rows, (1, 0, 2, 3)).reshape(blocks_all, EXPERTS * CAP, D)
    route = gate_weights / lax.optimization_barrier(jnp.sum(gate_weights, axis=-1, keepdims=True))
    route = route.reshape(blocks_all, TOK_DEV, TOP)

    def combine_pass(inputs):
        rows_back, slots_here, route_here = inputs
        picked = rows_back[slots_here].reshape(TOK_DEV, TOP, D).astype(jnp.float32)
        return jnp.einsum('tk,tkd->td', route_here, picked, precision=lax.Precision.HIGHEST).astype(jnp.bfloat16)
    moe_out = lax.map(combine_pass, (expert_rows, slot_index, route)).reshape(TOKENS, D)
    normed_in = norm_rows(tokens, input_gain).astype(jnp.bfloat16)
    projected = jnp.dot(normed_in, kv_weight, preferred_element_type=jnp.float32)
    half = KVH * HD
    keys = norm_rows(projected[:, :half].reshape(TOKENS, KVH, HD), key_gain).astype(jnp.bfloat16)
    values = projected[:, half:].reshape(TOKENS, KVH, HD).astype(jnp.bfloat16)
    row_tokens = TOK_DEV * N_DEC
    group = H // KVH
    scale = HD ** (-0.5)

    def slab_pass(inputs):
        slab_keys, slab_values, page_order, page_counts, owners, slab_query, slab_new = inputs
        owner_of = token_requests(page_order, page_counts)
        members = owner_of[None, :] == jnp.arange(REQ_ROW, dtype=jnp.int32)[:, None]
        members = members[:, None, None, :]
        queries = slab_query.reshape(REQ_ROW, KVH, group, HD).astype(jnp.float32)
        scores = jnp.einsum('rkgd,tkd->rkgt', queries, slab_keys.astype(jnp.float32), precision=lax.Precision.HIGHEST) * scale
        scores = jnp.where(members, scores, FLOOR_SCORE)
        new_keys = slab_new[:, :half].reshape(REQ_ROW, KVH, HD).astype(jnp.float32)
        new_values = slab_new[:, half:].reshape(REQ_ROW, KVH, HD).astype(jnp.float32)
        own_score = jnp.einsum('rkgd,rkd->rkg', queries, new_keys, precision=lax.Precision.HIGHEST) * scale
        peak = jnp.maximum(lax.optimization_barrier(jnp.max(scores, axis=-1)), own_score)
        weights = jnp.where(members, jnp.exp(scores - peak[..., None]), 0.0)
        own_weight = jnp.exp(own_score - peak)
        total = lax.optimization_barrier(jnp.sum(weights, axis=-1)) + own_weight
        mixed = jnp.einsum('rkgt,tkd->rkgd', weights, slab_values.astype(jnp.float32), precision=lax.Precision.HIGHEST)
        mixed = mixed + own_weight[..., None] * new_values[:, :, None, :]
        request_rows = (mixed / total[..., None]).reshape(REQ_ROW, H * HD).astype(jnp.bfloat16)

        def device_rows(device):
            targets, live = slot_requests(owners, device, RCAP)
            return jnp.where(live[:, None], request_rows[targets], jnp.zeros((), jnp.bfloat16))
        return jax.vmap(device_rows)(jnp.arange(N_DEC, dtype=jnp.int32))
    decode_out = lax.map(slab_pass, (keys.reshape(N_PRE, row_tokens, KVH, HD), values.reshape(N_PRE, row_tokens, KVH, HD), page_list, lengths, assignment.reshape(N_PRE, REQ_ROW), query.reshape(N_PRE, REQ_ROW, H * HD), new_kv.reshape(N_PRE, REQ_ROW, 2 * half))).reshape(SLOTS, H * HD)
    return (moe_out, decode_out)
```

```python
import functools

import jax
import jax.numpy as jnp
from jax import lax
from jax.experimental import pallas as pl
from jax.experimental.pallas import tpu as pltpu
from jax.sharding import PartitionSpec as P

MESH = pl.DeviceIdType.MESH

H = 32
KVH = 4
HD = 128
PAGE = 16
RCAP = 3


EPSILON = 1e-06
FLOOR_SCORE = -1e30


def all_in_one(shard, axis):
    leaves = jax.tree.leaves(shard)
    sequence = sorted(range(len(leaves)), key=lambda k: -leaves[k].size)
    width = (1, *leaves[sequence[0]].shape)[-1]
    lines = [
        jnp.pad(leaves[k].reshape(-1), (0, -leaves[k].size % width)).reshape(-1, width)
        for k in sequence
    ]
    both, at, found = (lax.all_gather(jnp.concatenate(lines), axis), 0, {})
    for k, line in zip(sequence, lines):
        section = both[:, at : at + len(line)].reshape(len(both), -1)
        found[k] = section[:, : leaves[k].size].reshape(-1, *leaves[k].shape)
        at += len(line)
    numbers = iter(range(len(leaves)))
    return jax.tree.map(lambda _: found[next(numbers)], shard)


def joined(part, axis, combine):
    gathered = all_in_one(part, axis)

    def take(source):
        return jax.tree.map(lambda a: lax.dynamic_index_in_dim(a, source, 0, False), gathered)

    return lax.fori_loop(
        1, lax.axis_size(axis), lambda source, state: combine(state, take(source)), take(0)
    )


def norm_rows(values, scales):
    values = values.astype(jnp.float32)
    factor = lax.rsqrt(jnp.mean(values * values, axis=-1, keepdims=True) + EPSILON)
    return values * factor * scales


def token_requests(page_order, page_counts):
    page_total = page_order.shape[0]
    request_ends = jnp.cumsum(page_counts)
    positions = jnp.arange(page_total, dtype=jnp.int32)
    owner_at = jnp.sum((positions[:, None] >= request_ends[None, :]).astype(jnp.int32), axis=1)
    matches = page_order[:, None] == positions[None, :]
    page_owner = jnp.sum(jnp.where(matches, owner_at[:, None], 0), axis=0)
    return jnp.repeat(page_owner, PAGE)


def slot_requests(owners, device, slot_count):
    request_count = owners.shape[0]
    is_mine = (owners == device).astype(jnp.int32)
    order_mine = jnp.cumsum(is_mine) - 1
    slot_hit = (is_mine[None, :] == 1) & (
        order_mine[None, :] == jnp.arange(slot_count, dtype=jnp.int32)[:, None]
    )
    targets = jnp.sum(
        jnp.where(slot_hit, jnp.arange(request_count, dtype=jnp.int32)[None, :], 0), axis=1
    )
    return (targets, jnp.any(slot_hit, axis=1))


def empty_state(count):
    group = H // KVH
    return (
        jnp.full((count, KVH, group), FLOOR_SCORE, jnp.float32),
        jnp.zeros((count, KVH, group), jnp.float32),
        jnp.zeros((count, KVH, group, HD), jnp.float32),
    )


def attend_block(state, queries, targets, live, piece, piece_owner):
    peak, total, mixed = state
    row_count = piece.shape[0]
    half = KVH * HD
    piece_keys = piece[:, :half].reshape(row_count, KVH, HD)
    piece_values = piece[:, half:].reshape(row_count, KVH, HD).astype(jnp.float32)
    scores = jnp.einsum(
        "skgd,tkd->skgt", queries, piece_keys, preferred_element_type=jnp.float32
    ) * HD ** (-0.5)
    members = ((piece_owner[None, :] == targets[:, None]) & live[:, None])[:, None, None, :]
    scores = jnp.where(members, scores, FLOOR_SCORE)
    raised = jnp.maximum(peak, jnp.max(scores, axis=-1))
    weights = jnp.where(members, jnp.exp(scores - raised[..., None]), 0.0)
    total = jnp.sum(weights, axis=-1)
    mixed = jnp.einsum("skgt,tkd->skgd", weights, piece_values, precision=lax.Precision.HIGHEST)
    return (raised, total, mixed)


def join(first, second):
    highest = jnp.maximum(first[0], second[0])
    first_part = jnp.exp(first[0] - highest)
    second_part = jnp.exp(second[0] - highest)
    return (
        highest,
        first[1] * first_part + second[1] * second_part,
        first[2] * first_part[..., None] + second[2] * second_part[..., None],
    )


def finish(state, queries, fresh):
    peak, total, mixed = state
    count = queries.shape[0]
    half = KVH * HD
    new_keys = fresh[:, :half].reshape(count, KVH, HD)
    new_values = fresh[:, half:].reshape(count, KVH, HD).astype(jnp.float32)
    own_score = jnp.einsum(
        "skgd,skd->skg", queries, new_keys, preferred_element_type=jnp.float32
    ) * HD ** (-0.5)
    highest = jnp.maximum(peak, own_score)
    old_part = jnp.exp(peak - highest)
    new_part = jnp.exp(own_score - highest)
    mixed = mixed * old_part[..., None] + new_part[..., None] * new_values[:, :, None, :]
    return (mixed / (total * old_part + new_part)[..., None]).reshape(count, H * HD)


def moe_kernel(
    n,
    cap,
    att,
    gain,
    meta,
    wg_hbm,
    wu_hbm,
    wd_hbm,
    out,
    wg,
    wu,
    wd,
    gathered,
    metas,
    keys,
    routes,
    outbox,
    inbox,
    hidden,
    results,
    combined,
    mix,
    tall,
    part,
    ring_out,
    ring_in,
    w_sem,
    ag_send,
    ag_recv,
    meta_send,
    meta_recv,
    out_send,
    out_recv,
    back_send,
    back_recv,
    rs_send,
    rs_recv,
):
    rows, width = att.shape
    top = meta.shape[0] // 2
    block = n * cap
    half_rows = rows // 2
    far = n // 2
    g, pre, x = lax.axis_index("groups"), lax.axis_index("pre"), lax.axis_index("dec")
    y, c = lax.div(pre, 2), lax.rem(pre, 2)
    f = x * (1 - c) + y * c
    s = y * (1 - c) + x * c

    def device(first, second, core, orient):
        first, second = lax.rem(first + 2 * n, n), lax.rem(second + 2 * n, n)
        at_x = first * (1 - orient) + second * orient
        at_y = second * (1 - orient) + first * orient
        return (g, at_y * 2 + core, at_x)

    def remote(source, target, send, recv, where):
        return pltpu.make_async_remote_copy(
            src_ref=source,
            dst_ref=target,
            send_sem=send,
            recv_sem=recv,
            device_id=where,
            device_id_type=MESH,
        )

    loads = [
        pltpu.make_async_copy(a, b, w_sem.at[k])
        for k, (a, b) in enumerate(((wg_hbm, wg), (wu_hbm, wu), (wd_hbm, wd)))
    ]
    for load in loads:
        load.start()

    barrier = pltpu.get_barrier_semaphore()
    everyone = [device(f, s, 1 - c, c)]
    for step in range(1, n):
        everyone += [device(f + step, s, core, c) for core in range(2)]
        everyone += [device(f, s + step, core, c) for core in range(2)]
    for where in everyone:
        pl.semaphore_signal(barrier, inc=1, device_id=where, device_id_type=MESH)

    values = att[...].astype(jnp.float32)
    factor = lax.rsqrt(jnp.mean(values * values, axis=-1, keepdims=True) + EPSILON)
    gathered[0] = (values * factor * gain[...]).astype(jnp.bfloat16)
    metas[0] = meta[...]
    pl.semaphore_wait(barrier, len(everyone))

    meta_copies = [
        remote(
            meta, metas.at[n - k], meta_send.at[k - 1], meta_recv.at[n - k - 1], device(f + k, s, c, c)
        )
        for k in range(1, n)
    ]

    def ag_copy(k, way, u):
        source = (n - (k - 1)) % n if way == 0 else k - 1
        target = n - k if way == 0 else k
        span = pl.ds(u * half_rows, half_rows)
        return remote(
            gathered.at[source, span],
            gathered.at[target, span],
            ag_send.at[k - 1, way, u],
            ag_recv.at[k - 1, way, u],
            device(f + (1 if way == 0 else -1), s, c, c),
        )

    def exists(k, way, u, short):
        return 1 <= k <= far and (k != short or u == way)

    for k in range(1, far + 1):
        for u in range(2):
            for way in range(2):
                if not exists(k, way, u, far):
                    continue
                if k > 1:
                    ag_copy(k - 1, way, u).wait_recv()
                ag_copy(k, way, u).start()
        if k == 1:
            for copy in meta_copies:
                copy.start()

    for copy in meta_copies:
        copy.wait_recv()
    row = lax.broadcasted_iota(jnp.int32, (2 * n, rows), 0)
    index, core = row >> 1, row & 1
    reach = (index + 1) >> 1
    second = (s + jnp.where((index & 1) == 1, reach, -reach) + n) & (n - 1)
    expert_x = f * (1 - c) + second * c
    expert_y = second * (1 - c) + f * c
    expert = ((expert_y * 2 + core) * n + expert_x).astype(jnp.float32)
    earlier = jnp.where(
        lax.broadcasted_iota(jnp.int32, (rows, rows), 0)
        < lax.broadcasted_iota(jnp.int32, (rows, rows), 1),
        1.0,
        0.0,
    ).astype(jnp.bfloat16)
    for source in range(n):
        known = metas[source]
        hit = jnp.zeros((2 * n, rows), jnp.float32)
        weight = jnp.zeros((2 * n, rows), jnp.float32)
        for k in range(top):
            same = known[k : k + 1] == expert
            hit = jnp.where(same, 1.0, hit)
            weight = jnp.where(same, known[top + k : top + k + 1], weight)
        rank = jnp.dot(hit.astype(jnp.bfloat16), earlier, preferred_element_type=jnp.float32)
        keys[:, source * rows : (source + 1) * rows] = jnp.where(
            hit > 0.0, rank + float(source * cap), -1.0
        )
        routes[:, source * rows : (source + 1) * rows] = weight

    for way in range(2):
        ag_copy(far - 1, way, 1 - way).wait_recv()
        ag_copy(far, way, way).wait_recv()

    def offset(index):
        return lax.div(index + 1, 2) * (2 * lax.rem(index, 2) - 1)

    def out_copy(index, core):
        return remote(
            outbox.at[index, core],
            inbox.at[index, c],
            out_send.at[index, core],
            out_recv.at[index, c],
            device(f, s + offset(index), core, c),
        )

    slot = lax.broadcasted_iota(jnp.int32, (block, n * rows), 0).astype(jnp.float32)

    def send_rows(index, carry):
        picks = jnp.concatenate(
            [
                jnp.where(slot == keys[pl.ds(2 * index + core, 1), :], 1.0, 0.0).astype(jnp.bfloat16)
                for core in range(2)
            ],
            axis=0,
        )
        picked = jnp.dot(
            picks, gathered[...].reshape(n * rows, width), preferred_element_type=jnp.float32
        ).astype(jnp.bfloat16)
        outbox[index] = picked.reshape(2, block, width)

        @pl.when(index == 0)
        def _():
            inbox[0, c] = outbox[0, c]
            out_copy(0, 1 - c).start()

        @pl.when(index > 0)
        def _():
            for core in range(2):
                out_copy(index, core).start()

        return carry

    lax.fori_loop(0, n, send_rows, 0)

    narrow = lax.broadcasted_iota(jnp.int32, (block, rows), 0).astype(jnp.float32)

    def weigh(source, carry):
        span = pl.ds(pl.multiple_of(source * rows, rows), rows)
        for e in range(2 * n):
            piece = jnp.where(narrow == keys[e : e + 1, span], routes[e : e + 1, span], 0.0)
            tall[e * block : (e + 1) * block] = piece
        whole = tall[...].T
        rounded = whole.astype(jnp.bfloat16)
        mix[source, 0:rows] = rounded
        mix[source, rows : 2 * rows] = (whole - rounded.astype(jnp.float32)).astype(jnp.bfloat16)
        return carry

    lax.fori_loop(0, n, weigh, 0)
    for load in loads:
        load.wait()

    def back_copy(index, core):
        first = f * (1 - c) + s * c
        at_x = first
        at_y = s * (1 - c) + f * c
        move = offset(index)
        where = (
            g,
            lax.rem(at_y - move * (1 - core) + n, n) * 2 + core,
            lax.rem(at_x - move * core + n, n),
        )
        return remote(
            results.at[index, core],
            combined.at[index, c],
            back_send.at[index, core],
            back_recv.at[index, c],
            where,
        )

    def out_arrival(index, core):
        return remote(
            outbox.at[index, core],
            inbox.at[index, core],
            out_send.at[index, core],
            out_recv.at[index, core],
            device(f, s, 1 - c, c),
        )

    def back_arrival(index, core):
        return remote(
            results.at[index, core],
            combined.at[index, core],
            back_send.at[index, core],
            back_recv.at[index, core],
            device(f, s, 1 - c, c),
        )

    hidden_width = wg.shape[1]
    tile = 256

    def work(b, carry):
        for j in range(4):
            index, core = 2 * b + j // 2, j % 2

            @pl.when((index > 0) | (core != c))
            def _(index=index, core=core):
                out_arrival(index, core).wait_recv()

        def first(t, inner):
            span = pl.ds(pl.multiple_of(t * tile, tile), tile)
            received = inbox[pl.ds(2 * b, 2)].reshape(4 * block, width)
            gate = jnp.dot(received, wg[:, span], preferred_element_type=jnp.float32)
            up = jnp.dot(received, wu[:, span], preferred_element_type=jnp.float32)
            hidden[:, span] = (gate / (1.0 + jnp.exp(-gate)) * up).astype(jnp.bfloat16)
            return inner

        lax.fori_loop(0, hidden_width // tile, first, 0)

        def second(t, inner):
            span = pl.ds(pl.multiple_of(t * tile, tile), tile)
            made = jnp.dot(hidden[...], wd[:, span], preferred_element_type=jnp.float32)
            results[pl.ds(2 * b, 2), :, :, span] = made.astype(jnp.bfloat16).reshape(
                2, 2, block, tile
            )
            return inner

        lax.fori_loop(0, width // tile, second, 0)

        @pl.when(b == 0)
        def _():
            combined[0, c] = results[0, c]

        for j in range(4):
            index, core = 2 * b + j // 2, j % 2

            @pl.when((index > 0) | (core != c))
            def _(index=index, core=core):
                back_copy(index, core).start()

        return carry

    lax.fori_loop(0, n // 2, work, 0)

    def arrive(index, carry):
        for core in range(2):

            @pl.when((index > 0) | (core != c))
            def _(core=core):
                back_arrival(index, core).wait_recv()

        return carry

    lax.fori_loop(0, n, arrive, 0)

    wide = 512

    def weighted(source, place):
        def piece(t, carry):
            span = pl.ds(pl.multiple_of(t * wide, wide), wide)
            both = jnp.dot(
                mix[source],
                combined[:, :, :, span].reshape(2 * n * block, wide),
                preferred_element_type=jnp.float32,
            )
            part[place * rows : (place + 1) * rows, span] = both[:rows] + both[rows:]
            return carry

        lax.fori_loop(0, width // wide, piece, 0)

    def rs_copy(k, way, u):
        span = pl.ds(u * half_rows, half_rows)
        return remote(
            ring_out.at[k - 1, way, span],
            ring_in.at[k - 1, way, span],
            rs_send.at[k - 1, way, u],
            rs_recv.at[k - 1, way, u],
            device(f + (1 if way == 0 else -1), s, c, c),
        )

    for k in range(1, far + 1):
        d = far + 1 - k
        weighted(d, 0)
        if k > 1:
            weighted(n - d, 1)
        for u in range(2):
            for way in range(2):
                if not exists(k, way, u, 1):
                    continue
                low, high = u * half_rows, (u + 1) * half_rows
                base = 0 if k == 1 else way * rows
                total = part[base + low : base + high]
                if exists(k - 1, way, u, 1):
                    rs_copy(k - 1, way, u).wait_recv()
                    total = total + ring_in[k - 2, way, low:high].astype(jnp.float32)
                ring_out[k - 1, way, low:high] = total.astype(jnp.bfloat16)
                rs_copy(k, way, u).start()
    weighted(0, 0)
    for u in range(2):
        low, high = u * half_rows, (u + 1) * half_rows
        total = part[low:high]
        for way in range(2):
            rs_copy(far, way, u).wait_recv()
            total = total + ring_in[far - 1, way, low:high].astype(jnp.float32)
        out[low:high] = total.astype(jnp.bfloat16)

    for copy in meta_copies:
        copy.wait_send()
    for k in range(1, far + 1):
        for u in range(2):
            for way in range(2):
                if exists(k, way, u, far):
                    ag_copy(k, way, u).wait_send()
                if exists(k, way, u, 1):
                    rs_copy(k, way, u).wait_send()

    def leave(index, carry):
        for core in range(2):

            @pl.when((index > 0) | (core != c))
            def _(core=core):
                out_copy(index, core).wait_send()
                back_copy(index, core).wait_send()

        return carry

    lax.fori_loop(0, n, leave, 0)


def expert_branch(attended, post_gain, w_gate, w_up, w_down, expert_ids, gate_weights):
    rows, width = attended.shape
    top = expert_ids.shape[1]
    inner = w_gate.shape[2]
    n = lax.axis_size("dec")
    experts = n * lax.axis_size("pre")
    cap = max(2, rows * top * 5 // (4 * experts))
    block = n * cap
    route = gate_weights / jnp.sum(gate_weights, axis=-1, keepdims=True)
    meta = jnp.concatenate([expert_ids.astype(jnp.float32), route], axis=1).T
    far = n // 2
    bf16, f32 = jnp.bfloat16, jnp.float32
    dma = pltpu.SemaphoreType.DMA
    vmem = pl.BlockSpec(memory_space=pltpu.VMEM)
    hbm = pl.BlockSpec(memory_space=pl.ANY)
    return pl.pallas_call(
        functools.partial(moe_kernel, n, cap),
        out_shape=jax.ShapeDtypeStruct((rows, width), bf16),
        in_specs=[vmem] * 3 + [hbm] * 3,
        out_specs=vmem,
        scratch_shapes=[
            pltpu.VMEM((width, inner), bf16),
            pltpu.VMEM((width, inner), bf16),
            pltpu.VMEM((inner, width), bf16),
            pltpu.VMEM((n, rows, width), bf16),
            pltpu.VMEM((n, 2 * top, rows), f32),
            pltpu.VMEM((2 * n, n * rows), f32),
            pltpu.VMEM((2 * n, n * rows), f32),
            pltpu.VMEM((n, 2, block, width), bf16),
            pltpu.VMEM((n, 2, block, width), bf16),
            pltpu.VMEM((4 * block, inner), bf16),
            pltpu.VMEM((n, 2, block, width), bf16),
            pltpu.VMEM((n, 2, block, width), bf16),
            pltpu.VMEM((n, 2 * rows, 2 * n * block), bf16),
            pltpu.VMEM((2 * n * block, rows), f32),
            pltpu.VMEM((2 * rows, width), f32),
            pltpu.VMEM((far, 2, rows, width), bf16),
            pltpu.VMEM((far, 2, rows, width), bf16),
            dma((3,)),
            dma((far, 2, 2)),
            dma((far, 2, 2)),
            dma((n - 1,)),
            dma((n - 1,)),
            dma((n, 2)),
            dma((n, 2)),
            dma((n, 2)),
            dma((n, 2)),
            dma((far, 2, 2)),
            dma((far, 2, 2)),
        ],
        compiler_params=pltpu.CompilerParams(
            collective_id=0, has_side_effects=True, vmem_limit_bytes=64 * 1024 * 1024 - 65536
        ),
        name="expert_branch",
    )(
        attended,
        post_gain.reshape(1, width),
        meta,
        w_gate.reshape(width, inner),
        w_up.reshape(width, inner),
        w_down.reshape(inner, width),
    )


def body(
    tokens,
    attended,
    input_gain,
    post_gain,
    kv_weight,
    key_gain,
    w_gate,
    w_up,
    w_down,
    expert_ids,
    gate_weights,
    page_list,
    lengths,
    assignment,
    query,
    new_kv,
):
    local_tokens = tokens.shape[0]
    model_width = tokens.shape[1]
    normed_in = norm_rows(tokens, input_gain).astype(jnp.bfloat16)
    projected = jnp.dot(
        normed_in,
        lax.all_gather(kv_weight, "pre", axis=0, tiled=True),
        preferred_element_type=jnp.float32,
    )
    half = KVH * HD
    keys = norm_rows(projected[:, :half].reshape(local_tokens, KVH, HD), key_gain).astype(
        jnp.bfloat16
    )
    cache = jnp.concatenate(
        [keys.reshape(local_tokens, half), projected[:, half:].astype(jnp.bfloat16)], axis=1
    )
    moe_out = expert_branch(
        attended, post_gain, w_gate, w_up, w_down, expert_ids, gate_weights
    )
    device = lax.axis_index("dec")
    owners = assignment[:, 0]
    request_count = owners.shape[0]
    owner_of = token_requests(page_list[0], lengths[0])
    targets, live = slot_requests(owners, device, RCAP)
    group = H // KVH
    everyone = query.reshape(request_count, KVH, group, HD)
    local_owner = lax.dynamic_slice_in_dim(owner_of, device * local_tokens, local_tokens, 0)
    partial_state = attend_block(
        empty_state(request_count),
        everyone,
        jnp.arange(request_count, dtype=jnp.int32),
        jnp.ones((request_count,), jnp.bool_),
        cache,
        local_owner,
    )
    state = joined(partial_state, "dec", join)
    request_rows = finish(state, everyone, new_kv).astype(jnp.bfloat16)
    decode_out = jnp.where(live[:, None], request_rows[targets], jnp.zeros((), jnp.bfloat16))
    return (moe_out, decode_out)


def solution(mesh):
    in_specs = (
        P(("groups", "pre", "dec"), None),
        P(("groups", "pre", "dec"), None),
        P(),
        P(),
        P("pre", None),
        P(),
        P(("pre", "dec"), None, None),
        P(("pre", "dec"), None, None),
        P(("pre", "dec"), None, None),
        P(("groups", "pre", "dec"), None),
        P(("groups", "pre", "dec"), None),
        P(("groups", "pre"), None),
        P(("groups", "pre"), None),
        P(("groups", "pre"), None),
        P(("groups", "pre"), None),
        P(("groups", "pre"), None),
    )
    out_specs = (P(("groups", "pre", "dec"), None), P(("groups", "pre", "dec"), None))
    return jax.shard_map(body, mesh=mesh, in_specs=in_specs, out_specs=out_specs, check_vma=False)
```

```python
import functools

import jax
import jax.numpy as jnp
from jax import lax
from jax.experimental import pallas as pl
from jax.experimental.pallas import tpu as pltpu
from jax.sharding import PartitionSpec as P

MESH = pl.DeviceIdType.MESH

H = 32
KVH = 4
HD = 128
PAGE = 16
RCAP = 3


EPSILON = 1e-06
FLOOR_SCORE = -1e30


def norm_rows(values, scales):
    values = values.astype(jnp.float32)
    factor = lax.rsqrt(jnp.mean(values * values, axis=-1, keepdims=True) + EPSILON)
    return values * factor * scales


def step_kernel(
    n,
    cap,
    att,
    gain,
    ids,
    gates,
    toks,
    in_gain,
    kvw,
    key_gain,
    pages,
    counts,
    owners,
    queries,
    fresh,
    wg_hbm,
    wu_hbm,
    wd_hbm,
    out,
    dec_out,
    wg,
    wu,
    wd,
    gathered,
    metas,
    keys,
    routes,
    outbox,
    inbox,
    hidden,
    results,
    combined,
    mix,
    tall,
    part,
    ring_out,
    ring_in,
    normed_in,
    kv_all,
    projected,
    mixes,
    peaks,
    states,
    arrived,
    w_sem,
    ag_send,
    ag_recv,
    meta_send,
    meta_recv,
    out_send,
    out_recv,
    back_send,
    back_recv,
    rs_send,
    rs_recv,
    kv_send,
    kv_recv,
    pair_send,
    pair_recv,
    dec_send,
    dec_recv,
):
    rows, width = att.shape
    top = ids.shape[0]
    block = n * cap
    half_rows = rows // 2
    far = n // 2
    last = n - 1
    main = 8
    extra = cap - main
    tail = n * main
    g, pre, x = lax.axis_index("groups"), lax.axis_index("pre"), lax.axis_index("dec")
    y, c = lax.div(pre, 2), lax.rem(pre, 2)
    f = x * (1 - c) + y * c
    s = y * (1 - c) + x * c

    def device(first, second, core, orient):
        first, second = lax.rem(first + 2 * n, n), lax.rem(second + 2 * n, n)
        at_x = first * (1 - orient) + second * orient
        at_y = second * (1 - orient) + first * orient
        return (g, at_y * 2 + core, at_x)

    def remote(source, target, send, recv, where):
        return pltpu.make_async_remote_copy(
            src_ref=source,
            dst_ref=target,
            send_sem=send,
            recv_sem=recv,
            device_id=where,
            device_id_type=MESH,
        )

    loads = [
        pltpu.make_async_copy(a, b, w_sem.at[k])
        for k, (a, b) in enumerate(((wg_hbm, wg), (wu_hbm, wu), (wd_hbm, wd)))
    ]
    for load in loads:
        load.start()

    barrier = pltpu.get_barrier_semaphore()
    everyone = [device(f, s, 1 - c, c)]
    for step in range(1, n):
        everyone += [device(f + step, s, core, c) for core in range(2)]
        everyone += [device(f, s + step, core, c) for core in range(2)]
    for where in everyone:
        pl.semaphore_signal(barrier, inc=1, device_id=where, device_id_type=MESH)

    gathered[0] = norm_rows(att[...], gain[...]).astype(jnp.bfloat16)
    share_of = gates[...] / jnp.sum(gates[...], axis=0, keepdims=True)
    metas[0, 0:top] = ids[...].astype(jnp.float32)
    metas[0, top : 2 * top] = share_of
    pl.semaphore_wait(barrier, len(everyone))

    kv_rows = kvw.shape[0]
    kv_half = kv_rows // 2
    partner = (g, y * 2 + 1 - c, x)

    def kv_copy(k, way):
        span = pl.ds(0, kv_rows) if k < far else pl.ds(way * kv_half, kv_half)
        move = -(k - 1) if way == 0 else k - 1
        block_at = lax.rem(y + move + n, n) * 2 + c
        where = (g, lax.rem(y + (1 if way == 0 else n - 1), n) * 2 + c, x)
        return remote(
            kvw if k == 1 else kv_all.at[block_at, span],
            kv_all.at[block_at, span],
            kv_send.at[k - 1, way],
            kv_recv.at[k - 1, way],
            where,
        )

    def pair_copy(index):
        block_at = lax.rem(y + index, n) * 2 + c
        return remote(
            kvw if index == 0 else kv_all.at[block_at],
            kv_all.at[block_at],
            pair_send.at[index],
            pair_recv.at[index],
            partner,
        )

    def kv_step(k):
        if k > 1:
            for way in range(2):
                kv_copy(k - 1, way).wait_recv()
        if k <= far:
            for way in range(2):
                kv_copy(k, way).start()
        if k == 1:
            pair_copy(0).start()
        elif k <= far:
            pair_copy(n - (k - 1)).start()
            pair_copy(k - 1).start()
        else:
            pair_copy(far).start()

    meta_copies = [
        remote(
            metas.at[0], metas.at[n - k], meta_send.at[k - 1], meta_recv.at[n - k - 1], device(f + k, s, c, c)
        )
        for k in range(1, n)
    ]

    def ag_copy(k, way, u):
        source = (n - (k - 1)) % n if way == 0 else k - 1
        target = n - k if way == 0 else k
        span = pl.ds(u * half_rows, half_rows)
        return remote(
            gathered.at[source, span],
            gathered.at[target, span],
            ag_send.at[k - 1, way, u],
            ag_recv.at[k - 1, way, u],
            device(f + (1 if way == 0 else -1), s, c, c),
        )

    def exists(k, way, u, short):
        return 1 <= k <= far and (k != short or u == way)

    for k in range(1, far + 1):
        for u in range(2):
            for way in range(2):
                if not exists(k, way, u, far):
                    continue
                if k > 1:
                    ag_copy(k - 1, way, u).wait_recv()
                ag_copy(k, way, u).start()
        if k == 1:
            for copy in meta_copies:
                copy.start()

        @pl.when(c == 0)
        def _(k=k):
            kv_step(k)


    kv_all[pre] = kvw[...]
    normed_in[...] = norm_rows(toks[...], in_gain[...]).astype(jnp.bfloat16)

    for copy in meta_copies:
        copy.wait_recv()
    row = lax.broadcasted_iota(jnp.int32, (2 * n, rows), 0)
    index, core = row >> 1, row & 1
    reach = jnp.where(index == last, 0, (index >> 1) + 1)
    second = (s + jnp.where((index & 1) == 1, -reach, reach) + n) & (n - 1)
    expert_x = f * (1 - c) + second * c
    expert_y = second * (1 - c) + f * c
    expert = ((expert_y * 2 + core) * n + expert_x).astype(jnp.float32)
    earlier = jnp.where(
        lax.broadcasted_iota(jnp.int32, (rows, rows), 0)
        < lax.broadcasted_iota(jnp.int32, (rows, rows), 1),
        1.0,
        0.0,
    ).astype(jnp.bfloat16)
    for source in range(n):
        known = metas[source]
        hit = jnp.zeros((2 * n, rows), jnp.float32)
        weight = jnp.zeros((2 * n, rows), jnp.float32)
        for k in range(top):
            same = known[k : k + 1] == expert
            hit = jnp.where(same, 1.0, hit)
            weight = jnp.where(same, known[top + k : top + k + 1], weight)
        rank = jnp.dot(hit.astype(jnp.bfloat16), earlier, preferred_element_type=jnp.float32)
        keys[:, source * rows : (source + 1) * rows] = jnp.where(
            hit > 0.0,
            jnp.where(
                rank < main, rank + float(source * main), rank + float(tail + source * extra - main)
            ),
            -1.0,
        )
        routes[:, source * rows : (source + 1) * rows] = weight

    for way in range(2):
        ag_copy(far - 1, way, 1 - way).wait_recv()
        ag_copy(far, way, way).wait_recv()

    def kv_turn(core, k):
        @pl.when(c == core)
        def _():
            kv_step(k)

    kv_turn(0, far + 1)
    kv_turn(1, 1)

    def offset(index):
        return (lax.div(index, 2) + 1) * (1 - 2 * lax.rem(index, 2)) * (1 - lax.div(index, n - 1))

    def out_copy(index, core):
        return remote(
            outbox.at[index, core],
            inbox.at[index, c],
            out_send.at[index, core],
            out_recv.at[index, c],
            device(f, s + offset(index), core, c),
        )

    slot = lax.broadcasted_iota(jnp.int32, (block, n * rows), 0).astype(jnp.float32)

    def send_rows(index, carry):
        picks = jnp.concatenate(
            [
                jnp.where(slot == keys[pl.ds(2 * index + core, 1), :], 1.0, 0.0).astype(jnp.bfloat16)
                for core in range(2)
            ],
            axis=0,
        )
        picked = jnp.dot(
            picks, gathered[...].reshape(n * rows, width), preferred_element_type=jnp.float32
        ).astype(jnp.bfloat16)
        outbox[index] = picked.reshape(2, block, width)

        @pl.when(index == last)
        def _():
            inbox[last, c] = outbox[last, c]
            out_copy(last, 1 - c).start()

        @pl.when(index < last)
        def _():
            for core in range(2):
                out_copy(index, core).start()

        return carry

    lax.fori_loop(0, n, send_rows, 0)
    kv_turn(1, 2)

    pair = 2 * main
    line = lax.broadcasted_iota(jnp.int32, (2 * pair, rows), 0)

    def weigh(source, carry):
        span = pl.ds(pl.multiple_of(source * rows, rows), rows)
        narrow = (
            line + jnp.where(line < pair, lax.div(source, 2) * pair, tail - pair)
        ).astype(jnp.float32)
        for e in range(2 * n):
            piece = jnp.where(narrow == keys[e : e + 1, span], routes[e : e + 1, span], 0.0)
            tall[e * pair : (e + 1) * pair] = piece[:pair]
            tall[(2 * n + e) * pair : (2 * n + e + 1) * pair] = piece[pair:]
        whole = tall[...].T
        rounded = whole.astype(jnp.bfloat16)
        mix[source, 0:rows] = rounded
        mix[source, rows : 2 * rows] = (whole - rounded.astype(jnp.float32)).astype(jnp.bfloat16)
        return carry

    lax.fori_loop(0, n, weigh, 0)
    kv_turn(1, 3)
    for load in loads:
        load.wait()

    def back_copy(index, core):
        first = f * (1 - c) + s * c
        at_x = first
        at_y = s * (1 - c) + f * c
        move = offset(index)
        where = (
            g,
            lax.rem(at_y - move * (1 - core) + n, n) * 2 + core,
            lax.rem(at_x - move * core + n, n),
        )
        return remote(
            results.at[index, core],
            combined.at[index, c],
            back_send.at[index, core],
            back_recv.at[index, c],
            where,
        )

    def out_arrival(index, core):
        return remote(
            outbox.at[index, core],
            inbox.at[index, core],
            out_send.at[index, core],
            out_recv.at[index, core],
            device(f, s, 1 - c, c),
        )

    def back_arrival(index, core):
        return remote(
            results.at[index, core],
            combined.at[index, core],
            back_send.at[index, core],
            back_recv.at[index, core],
            device(f, s, 1 - c, c),
        )

    hidden_width = wg.shape[1]
    tile = 256

    def work(b, carry):
        for j in range(4):
            index, core = 2 * b + j // 2, j % 2

            @pl.when((index < last) | (core != c))
            def _(index=index, core=core):
                out_arrival(index, core).wait_recv()

        def first(t, inner):
            span = pl.ds(pl.multiple_of(t * tile, tile), tile)
            received = inbox[pl.ds(2 * b, 2)].reshape(4 * block, width)
            gate = jnp.dot(received, wg[:, span], preferred_element_type=jnp.float32)
            up = jnp.dot(received, wu[:, span], preferred_element_type=jnp.float32)
            hidden[:, span] = (gate / (1.0 + jnp.exp(-gate)) * up).astype(jnp.bfloat16)
            return inner

        lax.fori_loop(0, hidden_width // tile, first, 0)

        def second(t, inner):
            span = pl.ds(pl.multiple_of(t * tile, tile), tile)
            made = jnp.dot(hidden[...], wd[:, span], preferred_element_type=jnp.float32)
            results[pl.ds(2 * b, 2), :, :, span] = made.astype(jnp.bfloat16).reshape(
                2, 2, block, tile
            )
            return inner

        lax.fori_loop(0, width // tile, second, 0)

        @pl.when(b == n // 2 - 1)
        def _():
            combined[last, c] = results[last, c]

        for j in range(4):
            index, core = 2 * b + j // 2, j % 2

            @pl.when((index < last) | (core != c))
            def _(index=index, core=core):
                back_copy(index, core).start()

        return carry

    work(0, 0)
    kv_turn(1, 4)
    work(1, 0)
    kv_turn(1, 5)
    for index in range(n):
        pair_copy(index).wait_recv()

    kv_tile = 256

    def project(t, carry):
        span = pl.ds(pl.multiple_of(t * kv_tile, kv_tile), kv_tile)
        projected[:, span] = jnp.dot(
            normed_in[...],
            kv_all[:, :, span].reshape(width, kv_tile),
            preferred_element_type=jnp.float32,
        )
        return carry

    kv_width = kvw.shape[1]
    lax.fori_loop(0, kv_width // kv_tile, project, 0)

    requests = owners.shape[1]
    group = H // KVH
    lane = lax.broadcasted_iota(jnp.int32, (1, rows), 1)
    page_of = x * (rows // PAGE) + lax.div(lane, PAGE)
    place = jnp.zeros((1, rows), jnp.int32)
    for p in range(pages.shape[1]):
        place = jnp.where(page_of == pages[0, p], p, place)
    owner_of = jnp.zeros((1, rows), jnp.int32)
    end = 0
    slots = []
    for r in range(requests):
        end = end + counts[0, r]
        owner_of = owner_of + jnp.where(place >= end, 1, 0)
        order = 0
        for other in range(r):
            order = order + jnp.where(owners[0, other] == owners[0, r], 1, 0)
        slots.append(owners[0, r] * RCAP + order)
    members = owner_of == (
        lax.div(lax.broadcasted_iota(jnp.int32, (requests * group, rows), 0), group)
    )
    asked = queries[...].astype(jnp.float32)
    by_head = asked.reshape(requests, KVH, group, HD)
    half = KVH * HD
    left = lax.broadcasted_iota(jnp.int32, (requests * group, HD), 1) < HD // 2
    for head in range(KVH):
        key = norm_rows(projected[:, head * HD : (head + 1) * HD], key_gain[...]).astype(
            jnp.bfloat16
        )
        value = projected[:, half + head * HD : half + (head + 1) * HD].astype(jnp.bfloat16)
        wanted = by_head[:, head].reshape(requests * group, HD).astype(jnp.bfloat16)
        scores = lax.dot_general(
            wanted, key, (((1,), (1,)), ((), ())), preferred_element_type=jnp.float32
        ) * HD ** (-0.5)
        scores = jnp.where(members, scores, FLOOR_SCORE)
        peak = jnp.max(scores, axis=-1, keepdims=True)
        weights = jnp.where(members, jnp.exp(scores - peak), 0.0)
        upper = weights.astype(jnp.bfloat16)
        lower = (weights - upper.astype(jnp.float32)).astype(jnp.bfloat16)
        mixed = jnp.dot(upper, value, preferred_element_type=jnp.float32) + jnp.dot(
            lower, value, preferred_element_type=jnp.float32
        )
        sums = jnp.sum(weights, axis=-1, keepdims=True)
        mixes[:, head] = mixed.reshape(requests, group, HD)
        peaks[:, head] = jnp.where(left, peak, sums).reshape(requests, group, HD)

    lines = RCAP * H
    diagonal = lax.broadcasted_iota(jnp.int32, (lines, HD), 0) == lax.broadcasted_iota(
        jnp.int32, (lines, HD), 1
    )

    def chosen(device_at, source):
        found = []
        for q in range(RCAP):
            value = 0.0
            for r in range(requests):
                here = jnp.where(slots[r] == device_at * RCAP + q, 1.0, 0.0)
                value = value + here * source(r)
            found.append(value)
        return jnp.concatenate(found, axis=0)

    def dec_copy(device_at):
        return remote(
            states.at[device_at],
            arrived.at[x],
            dec_send.at[device_at],
            dec_recv.at[x],
            (g, pre, device_at),
        )

    def dec_arrival(device_at):
        return remote(
            states.at[device_at],
            arrived.at[device_at],
            dec_send.at[device_at],
            dec_recv.at[device_at],
            (g, pre, device_at),
        )

    def share(step, carry):
        device_at = lax.rem(x + step, n)
        states[device_at, 0:lines] = chosen(device_at, lambda r: mixes[r].reshape(H, HD))
        both = chosen(device_at, lambda r: peaks[r].reshape(H, HD))
        top_row = jnp.sum(jnp.where(diagonal, both[:, 0:1], 0.0), axis=0, keepdims=True)
        sum_row = jnp.sum(jnp.where(diagonal, both[:, HD - 1 : HD], 0.0), axis=0, keepdims=True)
        states[device_at, lines : lines + 8] = jnp.concatenate(
            [top_row, sum_row, jnp.zeros((6, HD), jnp.float32)], axis=0
        )

        @pl.when(step > 0)
        def _():
            dec_copy(device_at).start()

        @pl.when(step == 0)
        def _():
            arrived[x] = states[x]

        return carry

    lax.fori_loop(0, n, share, 0)
    lax.fori_loop(n // 4, n // 2, work, 0)

    for step in range(1, n):
        dec_arrival(lax.rem(x + step, n)).wait_recv()

    def column(line):
        return jnp.sum(jnp.where(diagonal, line, 0.0), axis=1, keepdims=True)

    highest = arrived[0, lines : lines + 1]
    for source in range(1, n):
        highest = jnp.maximum(highest, arrived[source, lines : lines + 1])
    total = jnp.zeros((1, HD), jnp.float32)
    blended = jnp.zeros((lines, HD), jnp.float32)
    for source in range(n):
        scale = jnp.exp(arrived[source, lines : lines + 1] - highest)
        total = total + arrived[source, lines + 1 : lines + 2] * scale
        blended = blended + arrived[source, 0:lines] * column(scale)
    new = fresh[...].astype(jnp.float32)

    def spread(r, base):
        return jnp.concatenate(
            [
                jnp.broadcast_to(
                    new[r : r + 1, base + head * HD : base + (head + 1) * HD], (group, HD)
                )
                for head in range(KVH)
            ],
            axis=0,
        )

    my_queries = chosen(x, lambda r: asked[r * H : (r + 1) * H])
    my_keys = chosen(x, lambda r: spread(r, 0))
    my_values = chosen(x, lambda r: spread(r, half))
    live = chosen(x, lambda r: jnp.ones((H, HD), jnp.float32))
    own = jnp.sum(my_queries * my_keys, axis=-1, keepdims=True) * HD ** (-0.5)
    old_top = column(highest)
    final = jnp.maximum(old_top, own)
    old_part = jnp.exp(old_top - final)
    new_part = jnp.exp(own - final)
    made = (blended * old_part + new_part * my_values) / (column(total) * old_part + new_part)
    dec_out[...] = jnp.where(live > 0.0, made, 0.0).astype(jnp.bfloat16)

    def arrive(index, carry):
        for core in range(2):

            @pl.when((index < last) | (core != c))
            def _(core=core):
                back_arrival(index, core).wait_recv()

        return carry

    lax.fori_loop(0, n, arrive, 0)

    wide = 512

    def weighted(source, place):
        def piece(t, carry):
            span = pl.ds(pl.multiple_of(t * wide, wide), wide)
            low = source // 2 * pair
            both = jnp.dot(
                mix[source, :, 0 : 2 * n * pair],
                combined[:, :, low : low + pair, span].reshape(2 * n * pair, wide),
                preferred_element_type=jnp.float32,
            ) + jnp.dot(
                mix[source, :, 2 * n * pair :],
                combined[:, :, tail : tail + pair, span].reshape(2 * n * pair, wide),
                preferred_element_type=jnp.float32,
            )
            part[place * rows : (place + 1) * rows, span] = both[:rows] + both[rows:]
            return carry

        lax.fori_loop(0, width // wide, piece, 0)

    def rs_copy(k, way, u):
        span = pl.ds(u * half_rows, half_rows)
        return remote(
            ring_out.at[k - 1, way, span],
            ring_in.at[k - 1, way, span],
            rs_send.at[k - 1, way, u],
            rs_recv.at[k - 1, way, u],
            device(f + (1 if way == 0 else -1), s, c, c),
        )

    for k in range(1, far + 1):
        d = far + 1 - k
        weighted(d, 0)
        if k > 1:
            weighted(n - d, 1)
        for u in range(2):
            for way in range(2):
                if not exists(k, way, u, 1):
                    continue
                low, high = u * half_rows, (u + 1) * half_rows
                base = 0 if k == 1 else way * rows
                total = part[base + low : base + high]
                if exists(k - 1, way, u, 1):
                    rs_copy(k - 1, way, u).wait_recv()
                    total = total + ring_in[k - 2, way, low:high].astype(jnp.float32)
                ring_out[k - 1, way, low:high] = total.astype(jnp.bfloat16)
                rs_copy(k, way, u).start()
    weighted(0, 0)
    for u in range(2):
        low, high = u * half_rows, (u + 1) * half_rows
        total = part[low:high]
        for way in range(2):
            rs_copy(far, way, u).wait_recv()
            total = total + ring_in[far - 1, way, low:high].astype(jnp.float32)
        out[low:high] = total.astype(jnp.bfloat16)

    for copy in meta_copies:
        copy.wait_send()
    for k in range(1, far + 1):
        for u in range(2):
            for way in range(2):
                if exists(k, way, u, far):
                    ag_copy(k, way, u).wait_send()
                if exists(k, way, u, 1):
                    rs_copy(k, way, u).wait_send()

    def leave(index, carry):
        for core in range(2):

            @pl.when((index < last) | (core != c))
            def _(core=core):
                out_copy(index, core).wait_send()
                back_copy(index, core).wait_send()

        return carry

    lax.fori_loop(0, n, leave, 0)
    for k in range(1, far + 1):
        for way in range(2):
            kv_copy(k, way).wait_send()
    for index in range(n):
        pair_copy(index).wait_send()
    for step in range(1, n):
        dec_copy(lax.rem(x + step, n)).wait_send()


def body(
    tokens,
    attended,
    input_gain,
    post_gain,
    kv_weight,
    key_gain,
    w_gate,
    w_up,
    w_down,
    expert_ids,
    gate_weights,
    page_list,
    lengths,
    assignment,
    query,
    new_kv,
):
    rows, width = attended.shape
    top = expert_ids.shape[1]
    inner = w_gate.shape[2]
    n = lax.axis_size("dec")
    experts = n * lax.axis_size("pre")
    cap = max(2, rows * top * 5 // (4 * experts))
    block = n * cap
    far = n // 2
    bf16, f32 = jnp.bfloat16, jnp.float32
    dma = pltpu.SemaphoreType.DMA
    vmem = pl.BlockSpec(memory_space=pltpu.VMEM)
    hbm = pl.BlockSpec(memory_space=pl.ANY)
    smem = pl.BlockSpec(memory_space=pltpu.SMEM)
    requests = assignment.shape[0]
    lines = RCAP * H
    kv_rows, kv_width = kv_weight.shape
    moe_out, decode_out = pl.pallas_call(
        functools.partial(step_kernel, n, cap),
        out_shape=(
            jax.ShapeDtypeStruct((rows, width), bf16),
            jax.ShapeDtypeStruct((lines, HD), bf16),
        ),
        in_specs=[vmem] * 8 + [smem] * 3 + [vmem] * 2 + [hbm] * 3,
        out_specs=(vmem, vmem),
        scratch_shapes=[
            pltpu.VMEM((width, inner), bf16),
            pltpu.VMEM((width, inner), bf16),
            pltpu.VMEM((inner, width), bf16),
            pltpu.VMEM((n, rows, width), bf16),
            pltpu.VMEM((n, 2 * top, rows), f32),
            pltpu.VMEM((2 * n, n * rows), f32),
            pltpu.VMEM((2 * n, n * rows), f32),
            pltpu.VMEM((n, 2, block, width), bf16),
            pltpu.VMEM((n, 2, block, width), bf16),
            pltpu.VMEM((4 * block, inner), bf16),
            pltpu.VMEM((n, 2, block, width), bf16),
            pltpu.VMEM((n, 2, block, width), bf16),
            pltpu.VMEM((n, 2 * rows, 64 * n), bf16),
            pltpu.VMEM((64 * n, rows), f32),
            pltpu.VMEM((2 * rows, width), f32),
            pltpu.VMEM((far, 2, rows, width), bf16),
            pltpu.VMEM((far, 2, rows, width), bf16),
            pltpu.VMEM((rows, width), bf16),
            pltpu.VMEM((2 * n, kv_rows, kv_width), bf16),
            pltpu.VMEM((rows, kv_width), f32),
            pltpu.VMEM((requests, KVH, H // KVH, HD), f32),
            pltpu.VMEM((requests, KVH, H // KVH, HD), f32),
            pltpu.VMEM((n, lines + 8, HD), f32),
            pltpu.VMEM((n, lines + 8, HD), f32),
            dma((3,)),
            dma((far, 2, 2)),
            dma((far, 2, 2)),
            dma((n - 1,)),
            dma((n - 1,)),
            dma((n, 2)),
            dma((n, 2)),
            dma((n, 2)),
            dma((n, 2)),
            dma((far, 2, 2)),
            dma((far, 2, 2)),
            dma((far, 2)),
            dma((far, 2)),
            dma((n,)),
            dma((n,)),
            dma((n,)),
            dma((n,)),
        ],
        compiler_params=pltpu.CompilerParams(
            collective_id=0, has_side_effects=True, vmem_limit_bytes=64 * 1024 * 1024 - 65536
        ),
        name="whole_step",
    )(
        attended,
        post_gain.reshape(1, width),
        expert_ids.T,
        gate_weights.T,
        tokens,
        input_gain.reshape(1, width),
        kv_weight,
        key_gain.reshape(1, HD),
        page_list,
        lengths,
        assignment.T,
        query.reshape(requests * H, HD),
        new_kv,
        w_gate.reshape(width, inner),
        w_up.reshape(width, inner),
        w_down.reshape(inner, width),
    )
    return moe_out, decode_out.reshape(RCAP, H * HD)


def solution(mesh):
    in_specs = (
        P(("groups", "pre", "dec"), None),
        P(("groups", "pre", "dec"), None),
        P(),
        P(),
        P("pre", None),
        P(),
        P(("pre", "dec"), None, None),
        P(("pre", "dec"), None, None),
        P(("pre", "dec"), None, None),
        P(("groups", "pre", "dec"), None),
        P(("groups", "pre", "dec"), None),
        P(("groups", "pre"), None),
        P(("groups", "pre"), None),
        P(("groups", "pre"), None),
        P(("groups", "pre"), None),
        P(("groups", "pre"), None),
    )
    out_specs = (P(("groups", "pre", "dec"), None), P(("groups", "pre", "dec"), None))
    return jax.shard_map(body, mesh=mesh, in_specs=in_specs, out_specs=out_specs, check_vma=False)
```

```python
import functools

import jax
import jax.numpy as jnp
from jax import lax
from jax.experimental import pallas as pl
from jax.experimental.pallas import tpu as pltpu
from jax.sharding import PartitionSpec as P

MESH = pl.DeviceIdType.MESH

H = 32
KVH = 4
HD = 128
PAGE = 16
RCAP = 3


EPSILON = 1e-06
FLOOR_SCORE = -1e30


def norm_rows(values, scales):
    values = values.astype(jnp.float32)
    factor = lax.rsqrt(jnp.mean(values * values, axis=-1, keepdims=True) + EPSILON)
    return values * factor * scales


def place_results(moe, dec, moe_out, dec_out):
    moe_out[...] = moe[...]
    for h in range(H):
        dec_out[:, h * HD : (h + 1) * HD] = dec[pl.ds(h, RCAP, stride=H), :].astype(jnp.bfloat16)


def step_kernel(
    n,
    cap,
    att,
    gain,
    ids,
    gates,
    toks,
    in_gain,
    kvw,
    key_gain,
    pages,
    counts,
    owners,
    queries,
    fresh,
    wg_hbm,
    wu_hbm,
    wd_hbm,
    out,
    dec_out,
    wg,
    wu,
    wd,
    gathered,
    metas,
    keys,
    routes,
    outbox,
    inbox,
    hidden,
    results,
    combined,
    mix,
    tall,
    part,
    ring_out,
    ring_in,
    asked,
    normed_in,
    kv_all,
    projected,
    mixes,
    peaks,
    states,
    arrived,
    w_sem,
    ag_send,
    ag_recv,
    meta_send,
    meta_recv,
    out_send,
    out_recv,
    back_send,
    back_recv,
    rs_send,
    rs_recv,
    kv_send,
    kv_recv,
    pair_send,
    pair_recv,
    dec_send,
    dec_recv,
):
    rows, width = att.shape
    top = ids.shape[0]
    block = n * cap
    half_rows = rows // 2
    far = n // 2
    last = n - 1
    main = 8
    extra = cap - main
    tail = n * main
    g, pre, x = lax.axis_index("groups"), lax.axis_index("pre"), lax.axis_index("dec")
    y, c = lax.div(pre, 2), lax.rem(pre, 2)
    f = x * (1 - c) + y * c
    s = y * (1 - c) + x * c

    def device(first, second, core, orient):
        first, second = lax.rem(first + 2 * n, n), lax.rem(second + 2 * n, n)
        at_x = first * (1 - orient) + second * orient
        at_y = second * (1 - orient) + first * orient
        return (g, at_y * 2 + core, at_x)

    def remote(source, target, send, recv, where):
        return pltpu.make_async_remote_copy(
            src_ref=source,
            dst_ref=target,
            send_sem=send,
            recv_sem=recv,
            device_id=where,
            device_id_type=MESH,
        )

    loads = [
        pltpu.make_async_copy(a, b, w_sem.at[k])
        for k, (a, b) in enumerate(((wg_hbm, wg), (wu_hbm, wu), (wd_hbm, wd)))
    ]
    for load in loads:
        load.start()

    barrier = pltpu.get_barrier_semaphore()
    everyone = [device(f, s, 1 - c, c)]
    for step in range(1, n):
        everyone += [device(f + step, s, core, c) for core in range(2)]
        everyone += [device(f, s + step, core, c) for core in range(2)]
    for where in everyone:
        pl.semaphore_signal(barrier, inc=1, device_id=where, device_id_type=MESH)

    gathered[0] = norm_rows(att[...], gain[...]).astype(jnp.bfloat16)
    share_of = gates[...] / jnp.sum(gates[...], axis=0, keepdims=True)
    metas[0, 0:top] = ids[...].astype(jnp.float32)
    metas[0, top : 2 * top] = share_of
    pl.semaphore_wait(barrier, len(everyone))

    kv_rows = kvw.shape[0]
    kv_half = kv_rows // 2
    partner = (g, y * 2 + 1 - c, x)

    def kv_copy(k, way):
        span = pl.ds(0, kv_rows) if k < far else pl.ds(way * kv_half, kv_half)
        move = -(k - 1) if way == 0 else k - 1
        block_at = lax.rem(y + move + n, n) * 2 + c
        where = (g, lax.rem(y + (1 if way == 0 else n - 1), n) * 2 + c, x)
        return remote(
            kvw if k == 1 else kv_all.at[block_at, span],
            kv_all.at[block_at, span],
            kv_send.at[k - 1, way],
            kv_recv.at[k - 1, way],
            where,
        )

    def pair_copy(index):
        block_at = lax.rem(y + index, n) * 2 + c
        return remote(
            kvw if index == 0 else kv_all.at[block_at],
            kv_all.at[block_at],
            pair_send.at[index],
            pair_recv.at[index],
            partner,
        )

    def kv_step(k):
        if k > 1:
            for way in range(2):
                kv_copy(k - 1, way).wait_recv()
        if k <= far:
            for way in range(2):
                kv_copy(k, way).start()
        if k == 1:
            pair_copy(0).start()
        elif k <= far:
            pair_copy(n - (k - 1)).start()
            pair_copy(k - 1).start()
        else:
            pair_copy(far).start()

    meta_copies = [
        remote(
            metas.at[0], metas.at[n - k], meta_send.at[k - 1], meta_recv.at[n - k - 1], device(f + k, s, c, c)
        )
        for k in range(1, n)
    ]

    def ag_copy(k, way, u):
        source = (n - (k - 1)) % n if way == 0 else k - 1
        target = n - k if way == 0 else k
        span = pl.ds(u * half_rows, half_rows)
        return remote(
            gathered.at[source, span],
            gathered.at[target, span],
            ag_send.at[k - 1, way, u],
            ag_recv.at[k - 1, way, u],
            device(f + (1 if way == 0 else -1), s, c, c),
        )

    def exists(k, way, u, short):
        return 1 <= k <= far and (k != short or u == way)

    for k in range(1, far + 1):
        for u in range(2):
            for way in range(2):
                if not exists(k, way, u, far):
                    continue
                if k > 1:
                    ag_copy(k - 1, way, u).wait_recv()
                ag_copy(k, way, u).start()
        if k == 1:
            for copy in meta_copies:
                copy.start()

        @pl.when(c == 0)
        def _(k=k):
            kv_step(k)

    @pl.when(c == 1)
    def _():
        kv_step(1)


    kv_all[pre] = kvw[...]
    normed_in[...] = norm_rows(toks[...], in_gain[...]).astype(jnp.bfloat16)

    for copy in meta_copies:
        copy.wait_recv()
    row = lax.broadcasted_iota(jnp.int32, (2 * n, rows), 0)
    index, core = row >> 1, row & 1
    reach = jnp.where(index == last, 0, (index >> 1) + 1)
    second = (s + jnp.where((index & 1) == 1, -reach, reach) + n) & (n - 1)
    expert_x = f * (1 - c) + second * c
    expert_y = second * (1 - c) + f * c
    expert = ((expert_y * 2 + core) * n + expert_x).astype(jnp.float32)
    earlier = jnp.where(
        lax.broadcasted_iota(jnp.int32, (rows, rows), 0)
        < lax.broadcasted_iota(jnp.int32, (rows, rows), 1),
        1.0,
        0.0,
    ).astype(jnp.bfloat16)
    for source in range(n):
        known = metas[source]
        hit = jnp.zeros((2 * n, rows), jnp.float32)
        weight = jnp.zeros((2 * n, rows), jnp.float32)
        for k in range(top):
            same = known[k : k + 1] == expert
            hit = jnp.where(same, 1.0, hit)
            weight = jnp.where(same, known[top + k : top + k + 1], weight)
        rank = jnp.dot(hit.astype(jnp.bfloat16), earlier, preferred_element_type=jnp.float32)
        keys[:, source * rows : (source + 1) * rows] = jnp.where(
            hit > 0.0,
            jnp.where(
                rank < main, rank + float(source * main), rank + float(tail + source * extra - main)
            ),
            -1.0,
        )
        routes[:, source * rows : (source + 1) * rows] = weight

    for way in range(2):
        ag_copy(far - 1, way, 1 - way).wait_recv()
        ag_copy(far, way, way).wait_recv()

    def kv_turn(core, k):
        @pl.when(c == core)
        def _():
            kv_step(k)

    kv_turn(0, far + 1)

    def offset(index):
        return (lax.div(index, 2) + 1) * (1 - 2 * lax.rem(index, 2)) * (1 - lax.div(index, n - 1))

    def out_copy(index, core):
        return remote(
            outbox.at[index, core],
            inbox.at[index, c],
            out_send.at[index, core],
            out_recv.at[index, c],
            device(f, s + offset(index), core, c),
        )

    slot = lax.broadcasted_iota(jnp.int32, (block, n * rows), 0).astype(jnp.float32)

    def send_rows(index, carry):
        picks = jnp.concatenate(
            [
                jnp.where(slot == keys[pl.ds(2 * index + core, 1), :], 1.0, 0.0).astype(jnp.bfloat16)
                for core in range(2)
            ],
            axis=0,
        )
        picked = jnp.dot(
            picks, gathered[...].reshape(n * rows, width), preferred_element_type=jnp.float32
        ).astype(jnp.bfloat16)
        outbox[index] = picked.reshape(2, block, width)

        @pl.when(index == last)
        def _():
            inbox[last, c] = outbox[last, c]
            out_copy(last, 1 - c).start()

        @pl.when(index < last)
        def _():
            for core in range(2):
                out_copy(index, core).start()

        return carry

    lax.fori_loop(0, n, send_rows, 0)
    kv_turn(1, 2)

    pair = 2 * main
    line = lax.broadcasted_iota(jnp.int32, (2 * pair, rows), 0)

    def weigh(source, carry):
        span = pl.ds(pl.multiple_of(source * rows, rows), rows)
        narrow = (
            line + jnp.where(line < pair, lax.div(source, 2) * pair, tail - pair)
        ).astype(jnp.float32)
        for e in range(2 * n):
            piece = jnp.where(narrow == keys[e : e + 1, span], routes[e : e + 1, span], 0.0)
            tall[e * pair : (e + 1) * pair] = piece[:pair]
            tall[(2 * n + e) * pair : (2 * n + e + 1) * pair] = piece[pair:]
        whole = tall[...].T
        rounded = whole.astype(jnp.bfloat16)
        mix[source, 0:rows] = rounded
        mix[source, rows : 2 * rows] = (whole - rounded.astype(jnp.float32)).astype(jnp.bfloat16)
        return carry

    lax.fori_loop(0, n, weigh, 0)
    kv_turn(1, 3)
    for load in loads:
        load.wait()

    def back_copy(index, core):
        first = f * (1 - c) + s * c
        at_x = first
        at_y = s * (1 - c) + f * c
        move = offset(index)
        where = (
            g,
            lax.rem(at_y - move * (1 - core) + n, n) * 2 + core,
            lax.rem(at_x - move * core + n, n),
        )
        return remote(
            results.at[index, core],
            combined.at[index, c],
            back_send.at[index, core],
            back_recv.at[index, c],
            where,
        )

    def out_arrival(index, core):
        return remote(
            outbox.at[index, core],
            inbox.at[index, core],
            out_send.at[index, core],
            out_recv.at[index, core],
            device(f, s, 1 - c, c),
        )

    def back_arrival(index, core):
        return remote(
            results.at[index, core],
            combined.at[index, core],
            back_send.at[index, core],
            back_recv.at[index, core],
            device(f, s, 1 - c, c),
        )

    hidden_width = wg.shape[1]
    tile = 256

    def work(b, carry):
        for j in range(4):
            index, core = 2 * b + j // 2, j % 2

            @pl.when((index < last) | (core != c))
            def _(index=index, core=core):
                out_arrival(index, core).wait_recv()

        def first(t, inner):
            span = pl.ds(pl.multiple_of(t * tile, tile), tile)
            received = inbox[pl.ds(2 * b, 2)].reshape(4 * block, width)
            gate = jnp.dot(received, wg[:, span], preferred_element_type=jnp.float32)
            up = jnp.dot(received, wu[:, span], preferred_element_type=jnp.float32)
            hidden[:, span] = (gate / (1.0 + jnp.exp(-gate)) * up).astype(jnp.bfloat16)
            return inner

        lax.fori_loop(0, hidden_width // tile, first, 0)

        def second(t, inner):
            span = pl.ds(pl.multiple_of(t * tile, tile), tile)
            made = jnp.dot(hidden[...], wd[:, span], preferred_element_type=jnp.float32)
            results[pl.ds(2 * b, 2), :, :, span] = made.astype(jnp.bfloat16).reshape(
                2, 2, block, tile
            )
            return inner

        lax.fori_loop(0, width // tile, second, 0)

        @pl.when(b == n // 2 - 1)
        def _():
            combined[last, c] = results[last, c]

        for j in range(4):
            index, core = 2 * b + j // 2, j % 2

            @pl.when((index < last) | (core != c))
            def _(index=index, core=core):
                back_copy(index, core).start()

        return carry

    work(0, 0)
    kv_turn(1, 4)
    work(1, 0)
    kv_turn(1, 5)
    for index in range(n):
        pair_copy(index).wait_recv()

    kv_tile = 256

    def project(t, carry):
        span = pl.ds(pl.multiple_of(t * kv_tile, kv_tile), kv_tile)
        projected[:, span] = jnp.dot(
            normed_in[...],
            kv_all[:, :, span].reshape(width, kv_tile),
            preferred_element_type=jnp.float32,
        )
        return carry

    kv_width = kvw.shape[1]
    lax.fori_loop(0, kv_width // kv_tile, project, 0)

    requests = owners.shape[1]
    group = H // KVH
    lane = lax.broadcasted_iota(jnp.int32, (1, rows), 1)
    page_of = x * (rows // PAGE) + lax.div(lane, PAGE)
    place = jnp.zeros((1, rows), jnp.int32)
    for p in range(pages.shape[1]):
        place = jnp.where(page_of == pages[0, p], p, place)
    owner_of = jnp.zeros((1, rows), jnp.int32)
    end = 0
    slots = []
    for r in range(requests):
        end = end + counts[0, r]
        owner_of = owner_of + jnp.where(place >= end, 1, 0)
        order = 0
        for other in range(r):
            order = order + jnp.where(owners[0, other] == owners[0, r], 1, 0)
        slots.append(owners[0, r] * RCAP + order)
    members = owner_of == (
        lax.div(lax.broadcasted_iota(jnp.int32, (requests * group, rows), 0), group)
    )
    for h in range(H):
        asked[pl.ds(h, requests, stride=H), :] = queries[:, h * HD : (h + 1) * HD].astype(
            jnp.float32
        )
    by_head = asked[...].reshape(requests, KVH, group, HD)
    half = KVH * HD
    left = lax.broadcasted_iota(jnp.int32, (requests * group, HD), 1) < HD // 2
    for head in range(KVH):
        key = norm_rows(projected[:, head * HD : (head + 1) * HD], key_gain[...]).astype(
            jnp.bfloat16
        )
        value = projected[:, half + head * HD : half + (head + 1) * HD].astype(jnp.bfloat16)
        wanted = by_head[:, head].reshape(requests * group, HD).astype(jnp.bfloat16)
        scores = lax.dot_general(
            wanted, key, (((1,), (1,)), ((), ())), preferred_element_type=jnp.float32
        ) * HD ** (-0.5)
        scores = jnp.where(members, scores, FLOOR_SCORE)
        peak = jnp.max(scores, axis=-1, keepdims=True)
        weights = jnp.where(members, jnp.exp(scores - peak), 0.0)
        upper = weights.astype(jnp.bfloat16)
        lower = (weights - upper.astype(jnp.float32)).astype(jnp.bfloat16)
        mixed = jnp.dot(upper, value, preferred_element_type=jnp.float32) + jnp.dot(
            lower, value, preferred_element_type=jnp.float32
        )
        sums = jnp.sum(weights, axis=-1, keepdims=True)
        mixes[:, head] = mixed.reshape(requests, group, HD)
        peaks[:, head] = jnp.where(left, peak, sums).reshape(requests, group, HD)

    lines = RCAP * H
    diagonal = lax.broadcasted_iota(jnp.int32, (lines, HD), 0) == lax.broadcasted_iota(
        jnp.int32, (lines, HD), 1
    )

    def chosen(device_at, source):
        found = []
        for q in range(RCAP):
            value = 0.0
            for r in range(requests):
                here = jnp.where(slots[r] == device_at * RCAP + q, 1.0, 0.0)
                value = value + here * source(r)
            found.append(value)
        return jnp.concatenate(found, axis=0)

    def dec_copy(device_at):
        return remote(
            states.at[device_at],
            arrived.at[x],
            dec_send.at[device_at],
            dec_recv.at[x],
            (g, pre, device_at),
        )

    def dec_arrival(device_at):
        return remote(
            states.at[device_at],
            arrived.at[device_at],
            dec_send.at[device_at],
            dec_recv.at[device_at],
            (g, pre, device_at),
        )

    def share(step, carry):
        device_at = lax.rem(x + step, n)
        states[device_at, 0:lines] = chosen(device_at, lambda r: mixes[r].reshape(H, HD))
        both = chosen(device_at, lambda r: peaks[r].reshape(H, HD))
        top_row = jnp.sum(jnp.where(diagonal, both[:, 0:1], 0.0), axis=0, keepdims=True)
        sum_row = jnp.sum(jnp.where(diagonal, both[:, HD - 1 : HD], 0.0), axis=0, keepdims=True)
        states[device_at, lines : lines + 8] = jnp.concatenate(
            [top_row, sum_row, jnp.zeros((6, HD), jnp.float32)], axis=0
        )

        @pl.when(step > 0)
        def _():
            dec_copy(device_at).start()

        @pl.when(step == 0)
        def _():
            arrived[x] = states[x]

        return carry

    lax.fori_loop(0, n, share, 0)
    lax.fori_loop(n // 4, n // 2, work, 0)

    for step in range(1, n):
        dec_arrival(lax.rem(x + step, n)).wait_recv()

    def column(line):
        return jnp.sum(jnp.where(diagonal, line, 0.0), axis=1, keepdims=True)

    highest = arrived[0, lines : lines + 1]
    for source in range(1, n):
        highest = jnp.maximum(highest, arrived[source, lines : lines + 1])
    total = jnp.zeros((1, HD), jnp.float32)
    blended = jnp.zeros((lines, HD), jnp.float32)
    for source in range(n):
        scale = jnp.exp(arrived[source, lines : lines + 1] - highest)
        total = total + arrived[source, lines + 1 : lines + 2] * scale
        blended = blended + arrived[source, 0:lines] * column(scale)
    new = fresh[...].astype(jnp.float32)

    def spread(r, base):
        return jnp.concatenate(
            [
                jnp.broadcast_to(
                    new[r : r + 1, base + head * HD : base + (head + 1) * HD], (group, HD)
                )
                for head in range(KVH)
            ],
            axis=0,
        )

    my_queries = chosen(x, lambda r: asked[r * H : (r + 1) * H])
    my_keys = chosen(x, lambda r: spread(r, 0))
    my_values = chosen(x, lambda r: spread(r, half))
    live = chosen(x, lambda r: jnp.ones((H, HD), jnp.float32))
    own = jnp.sum(my_queries * my_keys, axis=-1, keepdims=True) * HD ** (-0.5)
    old_top = column(highest)
    final = jnp.maximum(old_top, own)
    old_part = jnp.exp(old_top - final)
    new_part = jnp.exp(own - final)
    made = (blended * old_part + new_part * my_values) / (column(total) * old_part + new_part)
    dec_out[...] = jnp.where(live > 0.0, made, 0.0)

    def arrive(index, carry):
        for core in range(2):

            @pl.when((index < last) | (core != c))
            def _(core=core):
                back_arrival(index, core).wait_recv()

        return carry

    lax.fori_loop(0, n, arrive, 0)

    wide = 512

    def weighted(source, place):
        def piece(t, carry):
            span = pl.ds(pl.multiple_of(t * wide, wide), wide)
            low = source // 2 * pair
            both = jnp.dot(
                mix[source, :, 0 : 2 * n * pair],
                combined[:, :, low : low + pair, span].reshape(2 * n * pair, wide),
                preferred_element_type=jnp.float32,
            ) + jnp.dot(
                mix[source, :, 2 * n * pair :],
                combined[:, :, tail : tail + pair, span].reshape(2 * n * pair, wide),
                preferred_element_type=jnp.float32,
            )
            part[place * rows : (place + 1) * rows, span] = both[:rows] + both[rows:]
            return carry

        lax.fori_loop(0, width // wide, piece, 0)

    def rs_copy(k, way, u):
        span = pl.ds(u * half_rows, half_rows)
        return remote(
            ring_out.at[k - 1, way, span],
            ring_in.at[k - 1, way, span],
            rs_send.at[k - 1, way, u],
            rs_recv.at[k - 1, way, u],
            device(f + (1 if way == 0 else -1), s, c, c),
        )

    for k in range(1, far + 1):
        d = far + 1 - k
        weighted(d, 0)
        if k > 1:
            weighted(n - d, 1)
        for u in range(2):
            for way in range(2):
                if not exists(k, way, u, 1):
                    continue
                low, high = u * half_rows, (u + 1) * half_rows
                base = 0 if k == 1 else way * rows
                total = part[base + low : base + high]
                if exists(k - 1, way, u, 1):
                    rs_copy(k - 1, way, u).wait_recv()
                    total = total + ring_in[k - 2, way, low:high].astype(jnp.float32)
                ring_out[k - 1, way, low:high] = total.astype(jnp.bfloat16)
                rs_copy(k, way, u).start()
    weighted(0, 0)
    for u in range(2):
        low, high = u * half_rows, (u + 1) * half_rows
        total = part[low:high]
        for way in range(2):
            rs_copy(far, way, u).wait_recv()
            total = total + ring_in[far - 1, way, low:high].astype(jnp.float32)
        out[low:high] = total.astype(jnp.bfloat16)

    for copy in meta_copies:
        copy.wait_send()
    for k in range(1, far + 1):
        for u in range(2):
            for way in range(2):
                if exists(k, way, u, far):
                    ag_copy(k, way, u).wait_send()
                if exists(k, way, u, 1):
                    rs_copy(k, way, u).wait_send()

    def leave(index, carry):
        for core in range(2):

            @pl.when((index < last) | (core != c))
            def _(core=core):
                out_copy(index, core).wait_send()
                back_copy(index, core).wait_send()

        return carry

    lax.fori_loop(0, n, leave, 0)
    for k in range(1, far + 1):
        for way in range(2):
            kv_copy(k, way).wait_send()
    for index in range(n):
        pair_copy(index).wait_send()
    for step in range(1, n):
        dec_copy(lax.rem(x + step, n)).wait_send()


def body(
    tokens,
    attended,
    input_gain,
    post_gain,
    kv_weight,
    key_gain,
    w_gate,
    w_up,
    w_down,
    expert_ids,
    gate_weights,
    page_list,
    lengths,
    assignment,
    query,
    new_kv,
):
    rows, width = attended.shape
    top = expert_ids.shape[1]
    inner = w_gate.shape[2]
    n = lax.axis_size("dec")
    experts = n * lax.axis_size("pre")
    cap = max(2, rows * top * 5 // (4 * experts))
    block = n * cap
    far = n // 2
    bf16, f32 = jnp.bfloat16, jnp.float32
    dma = pltpu.SemaphoreType.DMA
    vmem = pl.BlockSpec(memory_space=pltpu.VMEM)
    hbm = pl.BlockSpec(memory_space=pl.ANY)
    smem = pl.BlockSpec(memory_space=pltpu.SMEM)
    requests = assignment.shape[0]
    lines = RCAP * H
    kv_rows, kv_width = kv_weight.shape
    moe_out, decode_out = pl.pallas_call(
        functools.partial(step_kernel, n, cap),
        out_shape=(
            jax.ShapeDtypeStruct((rows, width), bf16),
            jax.ShapeDtypeStruct((lines, HD), f32),
        ),
        in_specs=[vmem] * 8 + [smem] * 3 + [vmem] * 2 + [hbm] * 3,
        out_specs=(vmem, vmem),
        scratch_shapes=[
            pltpu.VMEM((width, inner), bf16),
            pltpu.VMEM((width, inner), bf16),
            pltpu.VMEM((inner, width), bf16),
            pltpu.VMEM((n, rows, width), bf16),
            pltpu.VMEM((n, 2 * top, rows), f32),
            pltpu.VMEM((2 * n, n * rows), f32),
            pltpu.VMEM((2 * n, n * rows), f32),
            pltpu.VMEM((n, 2, block, width), bf16),
            pltpu.VMEM((n, 2, block, width), bf16),
            pltpu.VMEM((4 * block, inner), bf16),
            pltpu.VMEM((n, 2, block, width), bf16),
            pltpu.VMEM((n, 2, block, width), bf16),
            pltpu.VMEM((n, 2 * rows, 64 * n), bf16),
            pltpu.VMEM((64 * n, rows), f32),
            pltpu.VMEM((2 * rows, width), f32),
            pltpu.VMEM((far, 2, rows, width), bf16),
            pltpu.VMEM((far, 2, rows, width), bf16),
            pltpu.VMEM((requests * H, HD), f32),
            pltpu.VMEM((rows, width), bf16),
            pltpu.VMEM((2 * n, kv_rows, kv_width), bf16),
            pltpu.VMEM((rows, kv_width), f32),
            pltpu.VMEM((requests, KVH, H // KVH, HD), f32),
            pltpu.VMEM((requests, KVH, H // KVH, HD), f32),
            pltpu.VMEM((n, lines + 8, HD), f32),
            pltpu.VMEM((n, lines + 8, HD), f32),
            dma((3,)),
            dma((far, 2, 2)),
            dma((far, 2, 2)),
            dma((n - 1,)),
            dma((n - 1,)),
            dma((n, 2)),
            dma((n, 2)),
            dma((n, 2)),
            dma((n, 2)),
            dma((far, 2, 2)),
            dma((far, 2, 2)),
            dma((far, 2)),
            dma((far, 2)),
            dma((n,)),
            dma((n,)),
            dma((n,)),
            dma((n,)),
        ],
        compiler_params=pltpu.CompilerParams(
            collective_id=0, has_side_effects=True, vmem_limit_bytes=64 * 1024 * 1024 - 65536
        ),
        name="whole_step",
    )(
        attended,
        post_gain.reshape(1, width),
        expert_ids.T,
        gate_weights.T,
        tokens,
        input_gain.reshape(1, width),
        kv_weight,
        key_gain.reshape(1, HD),
        page_list,
        lengths,
        assignment.T,
        query,
        new_kv,
        w_gate.reshape(width, inner),
        w_up.reshape(width, inner),
        w_down.reshape(inner, width),
    )
    return pl.pallas_call(
        place_results,
        out_shape=(
            jax.ShapeDtypeStruct((rows, width), bf16),
            jax.ShapeDtypeStruct((RCAP, H * HD), bf16),
        ),
        in_specs=[vmem] * 2,
        out_specs=(vmem, vmem),
        compiler_params=pltpu.CompilerParams(vmem_limit_bytes=16 * 1024 * 1024),
        name="place_results",
    )(moe_out, decode_out)


def solution(mesh):
    in_specs = (
        P(("groups", "pre", "dec"), None),
        P(("groups", "pre", "dec"), None),
        P(),
        P(),
        P("pre", None),
        P(),
        P(("pre", "dec"), None, None),
        P(("pre", "dec"), None, None),
        P(("pre", "dec"), None, None),
        P(("groups", "pre", "dec"), None),
        P(("groups", "pre", "dec"), None),
        P(("groups", "pre"), None),
        P(("groups", "pre"), None),
        P(("groups", "pre"), None),
        P(("groups", "pre"), None),
        P(("groups", "pre"), None),
    )
    out_specs = (P(("groups", "pre", "dec"), None), P(("groups", "pre", "dec"), None))
    return jax.shard_map(body, mesh=mesh, in_specs=in_specs, out_specs=out_specs, check_vma=False)
```

```python
import functools

import jax
import jax.numpy as jnp
from jax import lax
from jax.experimental import pallas as pl
from jax.experimental.pallas import tpu as pltpu
from jax.sharding import PartitionSpec as P

MESH = pl.DeviceIdType.MESH

H = 32
KVH = 4
HD = 128
PAGE = 16
RCAP = 3


EPSILON = 1e-06
FLOOR_SCORE = -1e30


def norm_rows(values, scales):
    values = values.astype(jnp.float32)
    factor = lax.rsqrt(jnp.mean(values * values, axis=-1, keepdims=True) + EPSILON)
    return values * factor * scales


def place_results(moe, dec, moe_out, dec_out, held, sems):
    whole = pltpu.make_async_copy(moe, moe_out, sems.at[0])
    small = pltpu.make_async_copy(dec, held, sems.at[1])
    whole.start()
    small.start()
    small.wait()
    for h in range(H):
        dec_out[:, h * HD : (h + 1) * HD] = held[pl.ds(h, RCAP, stride=H), :].astype(jnp.bfloat16)
    whole.wait()


def step_kernel(
    n,
    cap,
    att,
    gain,
    ids,
    gates,
    toks,
    in_gain,
    kvw,
    key_gain,
    pages,
    counts,
    owners,
    queries,
    fresh,
    wg_hbm,
    wu_hbm,
    wd_hbm,
    out,
    dec_out,
    wg,
    wu,
    wd,
    gathered,
    metas,
    keys,
    routes,
    outbox,
    inbox,
    hidden,
    results,
    combined,
    mix,
    tall,
    part,
    ring_out,
    ring_in,
    asked,
    normed_in,
    kv_all,
    projected,
    mixes,
    peaks,
    states,
    arrived,
    w_sem,
    ag_send,
    ag_recv,
    meta_send,
    meta_recv,
    out_send,
    out_recv,
    back_send,
    back_recv,
    rs_send,
    rs_recv,
    kv_send,
    kv_recv,
    pair_send,
    pair_recv,
    dec_send,
    dec_recv,
):
    rows, width = att.shape
    top = ids.shape[0]
    block = n * cap
    half_rows = rows // 2
    far = n // 2
    last = n - 1
    main = 8
    extra = cap - main
    tail = n * main
    g, pre, x = lax.axis_index("groups"), lax.axis_index("pre"), lax.axis_index("dec")
    y, c = lax.div(pre, 2), lax.rem(pre, 2)
    f = x * (1 - c) + y * c
    s = y * (1 - c) + x * c

    def device(first, second, core, orient):
        first, second = lax.rem(first + 2 * n, n), lax.rem(second + 2 * n, n)
        at_x = first * (1 - orient) + second * orient
        at_y = second * (1 - orient) + first * orient
        return (g, at_y * 2 + core, at_x)

    def remote(source, target, send, recv, where):
        return pltpu.make_async_remote_copy(
            src_ref=source,
            dst_ref=target,
            send_sem=send,
            recv_sem=recv,
            device_id=where,
            device_id_type=MESH,
        )

    loads = [
        pltpu.make_async_copy(a, b, w_sem.at[k])
        for k, (a, b) in enumerate(((wg_hbm, wg), (wu_hbm, wu), (wd_hbm, wd)))
    ]
    for load in loads:
        load.start()

    barrier = pltpu.get_barrier_semaphore()
    everyone = [device(f, s, 1 - c, c)]
    for step in range(1, n):
        everyone += [device(f + step, s, core, c) for core in range(2)]
        everyone += [device(f, s + step, core, c) for core in range(2)]
    for where in everyone:
        pl.semaphore_signal(barrier, inc=1, device_id=where, device_id_type=MESH)

    gathered[0] = norm_rows(att[...], gain[...]).astype(jnp.bfloat16)
    share_of = gates[...] / jnp.sum(gates[...], axis=0, keepdims=True)
    metas[0, 0:top] = ids[...].astype(jnp.float32)
    metas[0, top : 2 * top] = share_of
    pl.semaphore_wait(barrier, len(everyone))

    kv_rows = kvw.shape[0]
    kv_half = kv_rows // 2
    partner = (g, y * 2 + 1 - c, x)

    def kv_copy(k, way):
        span = pl.ds(0, kv_rows) if k < far else pl.ds(way * kv_half, kv_half)
        move = -(k - 1) if way == 0 else k - 1
        block_at = lax.rem(y + move + n, n) * 2 + c
        where = (g, lax.rem(y + (1 if way == 0 else n - 1), n) * 2 + c, x)
        return remote(
            kvw if k == 1 else kv_all.at[block_at, span],
            kv_all.at[block_at, span],
            kv_send.at[k - 1, way],
            kv_recv.at[k - 1, way],
            where,
        )

    def pair_copy(index):
        block_at = lax.rem(y + index, n) * 2 + c
        return remote(
            kvw if index == 0 else kv_all.at[block_at],
            kv_all.at[block_at],
            pair_send.at[index],
            pair_recv.at[index],
            partner,
        )

    def kv_step(k):
        if k > 1:
            for way in range(2):
                kv_copy(k - 1, way).wait_recv()
        if k <= far:
            for way in range(2):
                kv_copy(k, way).start()
        if k == 1:
            pair_copy(0).start()
        elif k <= far:
            pair_copy(n - (k - 1)).start()
            pair_copy(k - 1).start()
        else:
            pair_copy(far).start()

    meta_copies = [
        remote(
            metas.at[0], metas.at[n - k], meta_send.at[k - 1], meta_recv.at[n - k - 1], device(f + k, s, c, c)
        )
        for k in range(1, n)
    ]

    def ag_copy(k, way, u):
        source = (n - (k - 1)) % n if way == 0 else k - 1
        target = n - k if way == 0 else k
        span = pl.ds(u * half_rows, half_rows)
        return remote(
            gathered.at[source, span],
            gathered.at[target, span],
            ag_send.at[k - 1, way, u],
            ag_recv.at[k - 1, way, u],
            device(f + (1 if way == 0 else -1), s, c, c),
        )

    def exists(k, way, u, short):
        return 1 <= k <= far and (k != short or u == way)

    for k in range(1, far + 1):
        for u in range(2):
            for way in range(2):
                if not exists(k, way, u, far):
                    continue
                if k > 1:
                    ag_copy(k - 1, way, u).wait_recv()
                ag_copy(k, way, u).start()
        if k == 1:
            for copy in meta_copies:
                copy.start()

        @pl.when(c == 0)
        def _(k=k):
            kv_step(k)

    @pl.when(c == 1)
    def _():
        kv_step(1)


    kv_all[pre] = kvw[...]
    normed_in[...] = norm_rows(toks[...], in_gain[...]).astype(jnp.bfloat16)

    for copy in meta_copies:
        copy.wait_recv()
    row = lax.broadcasted_iota(jnp.int32, (2 * n, rows), 0)
    index, core = row >> 1, row & 1
    reach = jnp.where(index == last, 0, (index >> 1) + 1)
    second = (s + jnp.where((index & 1) == 1, -reach, reach) + n) & (n - 1)
    expert_x = f * (1 - c) + second * c
    expert_y = second * (1 - c) + f * c
    expert = ((expert_y * 2 + core) * n + expert_x).astype(jnp.float32)
    earlier = jnp.where(
        lax.broadcasted_iota(jnp.int32, (rows, rows), 0)
        < lax.broadcasted_iota(jnp.int32, (rows, rows), 1),
        1.0,
        0.0,
    ).astype(jnp.bfloat16)
    for source in range(n):
        known = metas[source]
        hit = jnp.zeros((2 * n, rows), jnp.float32)
        weight = jnp.zeros((2 * n, rows), jnp.float32)
        for k in range(top):
            same = known[k : k + 1] == expert
            hit = jnp.where(same, 1.0, hit)
            weight = jnp.where(same, known[top + k : top + k + 1], weight)
        rank = jnp.dot(hit.astype(jnp.bfloat16), earlier, preferred_element_type=jnp.float32)
        keys[:, source * rows : (source + 1) * rows] = jnp.where(
            hit > 0.0,
            jnp.where(
                rank < main, rank + float(source * main), rank + float(tail + source * extra - main)
            ),
            -1.0,
        )
        routes[:, source * rows : (source + 1) * rows] = weight

    for way in range(2):
        ag_copy(far - 1, way, 1 - way).wait_recv()
        ag_copy(far, way, way).wait_recv()

    def kv_turn(core, k):
        @pl.when(c == core)
        def _():
            kv_step(k)

    kv_turn(0, far + 1)

    def offset(index):
        return (lax.div(index, 2) + 1) * (1 - 2 * lax.rem(index, 2)) * (1 - lax.div(index, n - 1))

    def out_copy(index, core):
        return remote(
            outbox.at[index, core],
            inbox.at[index, c],
            out_send.at[index, core],
            out_recv.at[index, c],
            device(f, s + offset(index), core, c),
        )

    slot = lax.broadcasted_iota(jnp.int32, (block, n * rows), 0).astype(jnp.float32)

    def send_rows(index, carry):
        picks = jnp.concatenate(
            [
                jnp.where(slot == keys[pl.ds(2 * index + core, 1), :], 1.0, 0.0).astype(jnp.bfloat16)
                for core in range(2)
            ],
            axis=0,
        )
        picked = jnp.dot(
            picks, gathered[...].reshape(n * rows, width), preferred_element_type=jnp.float32
        ).astype(jnp.bfloat16)
        outbox[index] = picked.reshape(2, block, width)

        @pl.when(index == last)
        def _():
            inbox[last, c] = outbox[last, c]
            out_copy(last, 1 - c).start()

        @pl.when(index < last)
        def _():
            for core in range(2):
                out_copy(index, core).start()

        return carry

    lax.fori_loop(0, n, send_rows, 0)
    kv_turn(1, 2)

    pair = 2 * main
    line = lax.broadcasted_iota(jnp.int32, (2 * pair, rows), 0)

    def weigh(source, carry):
        span = pl.ds(pl.multiple_of(source * rows, rows), rows)
        narrow = (
            line + jnp.where(line < pair, lax.div(source, 2) * pair, tail - pair)
        ).astype(jnp.float32)
        for e in range(2 * n):
            piece = jnp.where(narrow == keys[e : e + 1, span], routes[e : e + 1, span], 0.0)
            tall[e * pair : (e + 1) * pair] = piece[:pair]
            tall[(2 * n + e) * pair : (2 * n + e + 1) * pair] = piece[pair:]
        whole = tall[...].T
        rounded = whole.astype(jnp.bfloat16)
        mix[source, 0:rows] = rounded
        mix[source, rows : 2 * rows] = (whole - rounded.astype(jnp.float32)).astype(jnp.bfloat16)
        return carry

    lax.fori_loop(0, n, weigh, 0)
    kv_turn(1, 3)
    for load in loads:
        load.wait()

    def back_copy(index, core):
        first = f * (1 - c) + s * c
        at_x = first
        at_y = s * (1 - c) + f * c
        move = offset(index)
        where = (
            g,
            lax.rem(at_y - move * (1 - core) + n, n) * 2 + core,
            lax.rem(at_x - move * core + n, n),
        )
        return remote(
            results.at[index, core],
            combined.at[index, c],
            back_send.at[index, core],
            back_recv.at[index, c],
            where,
        )

    def out_arrival(index, core):
        return remote(
            outbox.at[index, core],
            inbox.at[index, core],
            out_send.at[index, core],
            out_recv.at[index, core],
            device(f, s, 1 - c, c),
        )

    def back_arrival(index, core):
        return remote(
            results.at[index, core],
            combined.at[index, core],
            back_send.at[index, core],
            back_recv.at[index, core],
            device(f, s, 1 - c, c),
        )

    hidden_width = wg.shape[1]
    tile = 256

    def work(b, carry):
        for j in range(4):
            index, core = 2 * b + j // 2, j % 2

            @pl.when((index < last) | (core != c))
            def _(index=index, core=core):
                out_arrival(index, core).wait_recv()

        def first(t, inner):
            span = pl.ds(pl.multiple_of(t * tile, tile), tile)
            received = inbox[pl.ds(2 * b, 2)].reshape(4 * block, width)
            gate = jnp.dot(received, wg[:, span], preferred_element_type=jnp.float32)
            up = jnp.dot(received, wu[:, span], preferred_element_type=jnp.float32)
            hidden[:, span] = (gate / (1.0 + jnp.exp(-gate)) * up).astype(jnp.bfloat16)
            return inner

        lax.fori_loop(0, hidden_width // tile, first, 0)

        def second(t, inner):
            span = pl.ds(pl.multiple_of(t * tile, tile), tile)
            made = jnp.dot(hidden[...], wd[:, span], preferred_element_type=jnp.float32)
            results[pl.ds(2 * b, 2), :, :, span] = made.astype(jnp.bfloat16).reshape(
                2, 2, block, tile
            )
            return inner

        lax.fori_loop(0, width // tile, second, 0)

        @pl.when(b == n // 2 - 1)
        def _():
            combined[last, c] = results[last, c]

        for j in range(4):
            index, core = 2 * b + j // 2, j % 2

            @pl.when((index < last) | (core != c))
            def _(index=index, core=core):
                back_copy(index, core).start()

        return carry

    work(0, 0)
    kv_turn(1, 4)
    work(1, 0)
    kv_turn(1, 5)
    for index in range(n):
        pair_copy(index).wait_recv()

    kv_tile = 256

    def project(t, carry):
        span = pl.ds(pl.multiple_of(t * kv_tile, kv_tile), kv_tile)
        projected[:, span] = jnp.dot(
            normed_in[...],
            kv_all[:, :, span].reshape(width, kv_tile),
            preferred_element_type=jnp.float32,
        )
        return carry

    kv_width = kvw.shape[1]
    lax.fori_loop(0, kv_width // kv_tile, project, 0)

    requests = owners.shape[1]
    group = H // KVH
    lane = lax.broadcasted_iota(jnp.int32, (1, rows), 1)
    page_of = x * (rows // PAGE) + lax.div(lane, PAGE)
    place = jnp.zeros((1, rows), jnp.int32)
    for p in range(pages.shape[1]):
        place = jnp.where(page_of == pages[0, p], p, place)
    owner_of = jnp.zeros((1, rows), jnp.int32)
    end = 0
    slots = []
    for r in range(requests):
        end = end + counts[0, r]
        owner_of = owner_of + jnp.where(place >= end, 1, 0)
        order = 0
        for other in range(r):
            order = order + jnp.where(owners[0, other] == owners[0, r], 1, 0)
        slots.append(owners[0, r] * RCAP + order)
    members = owner_of == (
        lax.div(lax.broadcasted_iota(jnp.int32, (requests * group, rows), 0), group)
    )
    for h in range(H):
        asked[pl.ds(h, requests, stride=H), :] = queries[:, h * HD : (h + 1) * HD].astype(
            jnp.float32
        )
    by_head = asked[...].reshape(requests, KVH, group, HD)
    half = KVH * HD
    left = lax.broadcasted_iota(jnp.int32, (requests * group, HD), 1) < HD // 2
    for head in range(KVH):
        key = norm_rows(projected[:, head * HD : (head + 1) * HD], key_gain[...]).astype(
            jnp.bfloat16
        )
        value = projected[:, half + head * HD : half + (head + 1) * HD].astype(jnp.bfloat16)
        wanted = by_head[:, head].reshape(requests * group, HD).astype(jnp.bfloat16)
        scores = lax.dot_general(
            wanted, key, (((1,), (1,)), ((), ())), preferred_element_type=jnp.float32
        ) * HD ** (-0.5)
        scores = jnp.where(members, scores, FLOOR_SCORE)
        peak = jnp.max(scores, axis=-1, keepdims=True)
        weights = jnp.where(members, jnp.exp(scores - peak), 0.0)
        upper = weights.astype(jnp.bfloat16)
        lower = (weights - upper.astype(jnp.float32)).astype(jnp.bfloat16)
        mixed = jnp.dot(upper, value, preferred_element_type=jnp.float32) + jnp.dot(
            lower, value, preferred_element_type=jnp.float32
        )
        sums = jnp.sum(weights, axis=-1, keepdims=True)
        mixes[:, head] = mixed.reshape(requests, group, HD)
        peaks[:, head] = jnp.where(left, peak, sums).reshape(requests, group, HD)

    lines = RCAP * H
    diagonal = lax.broadcasted_iota(jnp.int32, (lines, HD), 0) == lax.broadcasted_iota(
        jnp.int32, (lines, HD), 1
    )

    def chosen(device_at, source):
        found = []
        for q in range(RCAP):
            value = 0.0
            for r in range(requests):
                here = jnp.where(slots[r] == device_at * RCAP + q, 1.0, 0.0)
                value = value + here * source(r)
            found.append(value)
        return jnp.concatenate(found, axis=0)

    def dec_copy(device_at):
        return remote(
            states.at[device_at],
            arrived.at[x],
            dec_send.at[device_at],
            dec_recv.at[x],
            (g, pre, device_at),
        )

    def dec_arrival(device_at):
        return remote(
            states.at[device_at],
            arrived.at[device_at],
            dec_send.at[device_at],
            dec_recv.at[device_at],
            (g, pre, device_at),
        )

    def share(step, carry):
        device_at = lax.rem(x + step, n)
        states[device_at, 0:lines] = chosen(device_at, lambda r: mixes[r].reshape(H, HD))
        both = chosen(device_at, lambda r: peaks[r].reshape(H, HD))
        top_row = jnp.sum(jnp.where(diagonal, both[:, 0:1], 0.0), axis=0, keepdims=True)
        sum_row = jnp.sum(jnp.where(diagonal, both[:, HD - 1 : HD], 0.0), axis=0, keepdims=True)
        states[device_at, lines : lines + 8] = jnp.concatenate(
            [top_row, sum_row, jnp.zeros((6, HD), jnp.float32)], axis=0
        )

        @pl.when(step > 0)
        def _():
            dec_copy(device_at).start()

        @pl.when(step == 0)
        def _():
            arrived[x] = states[x]

        return carry

    lax.fori_loop(0, n, share, 0)
    lax.fori_loop(n // 4, n // 2, work, 0)

    for step in range(1, n):
        dec_arrival(lax.rem(x + step, n)).wait_recv()

    def column(line):
        return jnp.sum(jnp.where(diagonal, line, 0.0), axis=1, keepdims=True)

    highest = arrived[0, lines : lines + 1]
    for source in range(1, n):
        highest = jnp.maximum(highest, arrived[source, lines : lines + 1])
    total = jnp.zeros((1, HD), jnp.float32)
    blended = jnp.zeros((lines, HD), jnp.float32)
    for source in range(n):
        scale = jnp.exp(arrived[source, lines : lines + 1] - highest)
        total = total + arrived[source, lines + 1 : lines + 2] * scale
        blended = blended + arrived[source, 0:lines] * column(scale)
    new = fresh[...].astype(jnp.float32)

    def spread(r, base):
        return jnp.concatenate(
            [
                jnp.broadcast_to(
                    new[r : r + 1, base + head * HD : base + (head + 1) * HD], (group, HD)
                )
                for head in range(KVH)
            ],
            axis=0,
        )

    my_queries = chosen(x, lambda r: asked[r * H : (r + 1) * H])
    my_keys = chosen(x, lambda r: spread(r, 0))
    my_values = chosen(x, lambda r: spread(r, half))
    live = chosen(x, lambda r: jnp.ones((H, HD), jnp.float32))
    own = jnp.sum(my_queries * my_keys, axis=-1, keepdims=True) * HD ** (-0.5)
    old_top = column(highest)
    final = jnp.maximum(old_top, own)
    old_part = jnp.exp(old_top - final)
    new_part = jnp.exp(own - final)
    made = (blended * old_part + new_part * my_values) / (column(total) * old_part + new_part)
    dec_out[...] = jnp.where(live > 0.0, made, 0.0)

    def arrive(index, carry):
        for core in range(2):

            @pl.when((index < last) | (core != c))
            def _(core=core):
                back_arrival(index, core).wait_recv()

        return carry

    lax.fori_loop(0, n, arrive, 0)

    wide = 512

    def weighted(source, place):
        def piece(t, carry):
            span = pl.ds(pl.multiple_of(t * wide, wide), wide)
            low = source // 2 * pair
            both = jnp.dot(
                mix[source, :, 0 : 2 * n * pair],
                combined[:, :, low : low + pair, span].reshape(2 * n * pair, wide),
                preferred_element_type=jnp.float32,
            ) + jnp.dot(
                mix[source, :, 2 * n * pair :],
                combined[:, :, tail : tail + pair, span].reshape(2 * n * pair, wide),
                preferred_element_type=jnp.float32,
            )
            part[place * rows : (place + 1) * rows, span] = both[:rows] + both[rows:]
            return carry

        lax.fori_loop(0, width // wide, piece, 0)

    def rs_copy(k, way, u):
        span = pl.ds(u * half_rows, half_rows)
        return remote(
            ring_out.at[k - 1, way, span],
            ring_in.at[k - 1, way, span],
            rs_send.at[k - 1, way, u],
            rs_recv.at[k - 1, way, u],
            device(f + (1 if way == 0 else -1), s, c, c),
        )

    for k in range(1, far + 1):
        d = far + 1 - k
        weighted(d, 0)
        if k > 1:
            weighted(n - d, 1)
        for turn in range(2):
            for way in range(2):
                u = way if turn else 1 - way
                if not exists(k, way, u, 1):
                    continue
                low, high = u * half_rows, (u + 1) * half_rows
                base = 0 if k == 1 else way * rows
                total = part[base + low : base + high]
                if exists(k - 1, way, u, 1):
                    rs_copy(k - 1, way, u).wait_recv()
                    total = total + ring_in[k - 2, way, low:high].astype(jnp.float32)
                ring_out[k - 1, way, low:high] = total.astype(jnp.bfloat16)
                rs_copy(k, way, u).start()
    weighted(0, 0)
    for u in range(2):
        low, high = u * half_rows, (u + 1) * half_rows
        total = part[low:high]
        for way in range(2):
            rs_copy(far, way, u).wait_recv()
            total = total + ring_in[far - 1, way, low:high].astype(jnp.float32)
        out[low:high] = total.astype(jnp.bfloat16)

    for copy in meta_copies:
        copy.wait_send()
    for k in range(1, far + 1):
        for u in range(2):
            for way in range(2):
                if exists(k, way, u, far):
                    ag_copy(k, way, u).wait_send()
                if exists(k, way, u, 1):
                    rs_copy(k, way, u).wait_send()

    def leave(index, carry):
        for core in range(2):

            @pl.when((index < last) | (core != c))
            def _(core=core):
                out_copy(index, core).wait_send()
                back_copy(index, core).wait_send()

        return carry

    lax.fori_loop(0, n, leave, 0)
    for k in range(1, far + 1):
        for way in range(2):
            kv_copy(k, way).wait_send()
    for index in range(n):
        pair_copy(index).wait_send()
    for step in range(1, n):
        dec_copy(lax.rem(x + step, n)).wait_send()


def body(
    tokens,
    attended,
    input_gain,
    post_gain,
    kv_weight,
    key_gain,
    w_gate,
    w_up,
    w_down,
    expert_ids,
    gate_weights,
    page_list,
    lengths,
    assignment,
    query,
    new_kv,
):
    rows, width = attended.shape
    top = expert_ids.shape[1]
    inner = w_gate.shape[2]
    n = lax.axis_size("dec")
    experts = n * lax.axis_size("pre")
    cap = max(2, rows * top * 5 // (4 * experts))
    block = n * cap
    far = n // 2
    bf16, f32 = jnp.bfloat16, jnp.float32
    dma = pltpu.SemaphoreType.DMA
    vmem = pl.BlockSpec(memory_space=pltpu.VMEM)
    hbm = pl.BlockSpec(memory_space=pl.ANY)
    smem = pl.BlockSpec(memory_space=pltpu.SMEM)
    requests = assignment.shape[0]
    lines = RCAP * H
    kv_rows, kv_width = kv_weight.shape
    moe_out, decode_out = pl.pallas_call(
        functools.partial(step_kernel, n, cap),
        out_shape=(
            jax.ShapeDtypeStruct((rows, width), bf16),
            jax.ShapeDtypeStruct((lines, HD), f32),
        ),
        in_specs=[vmem] * 8 + [smem] * 3 + [vmem] * 2 + [hbm] * 3,
        out_specs=(vmem, vmem),
        scratch_shapes=[
            pltpu.VMEM((width, inner), bf16),
            pltpu.VMEM((width, inner), bf16),
            pltpu.VMEM((inner, width), bf16),
            pltpu.VMEM((n, rows, width), bf16),
            pltpu.VMEM((n, 2 * top, rows), f32),
            pltpu.VMEM((2 * n, n * rows), f32),
            pltpu.VMEM((2 * n, n * rows), f32),
            pltpu.VMEM((n, 2, block, width), bf16),
            pltpu.VMEM((n, 2, block, width), bf16),
            pltpu.VMEM((4 * block, inner), bf16),
            pltpu.VMEM((n, 2, block, width), bf16),
            pltpu.VMEM((n, 2, block, width), bf16),
            pltpu.VMEM((n, 2 * rows, 64 * n), bf16),
            pltpu.VMEM((64 * n, rows), f32),
            pltpu.VMEM((2 * rows, width), f32),
            pltpu.VMEM((far, 2, rows, width), bf16),
            pltpu.VMEM((far, 2, rows, width), bf16),
            pltpu.VMEM((requests * H, HD), f32),
            pltpu.VMEM((rows, width), bf16),
            pltpu.VMEM((2 * n, kv_rows, kv_width), bf16),
            pltpu.VMEM((rows, kv_width), f32),
            pltpu.VMEM((requests, KVH, H // KVH, HD), f32),
            pltpu.VMEM((requests, KVH, H // KVH, HD), f32),
            pltpu.VMEM((n, lines + 8, HD), f32),
            pltpu.VMEM((n, lines + 8, HD), f32),
            dma((3,)),
            dma((far, 2, 2)),
            dma((far, 2, 2)),
            dma((n - 1,)),
            dma((n - 1,)),
            dma((n, 2)),
            dma((n, 2)),
            dma((n, 2)),
            dma((n, 2)),
            dma((far, 2, 2)),
            dma((far, 2, 2)),
            dma((far, 2)),
            dma((far, 2)),
            dma((n,)),
            dma((n,)),
            dma((n,)),
            dma((n,)),
        ],
        compiler_params=pltpu.CompilerParams(
            collective_id=0, has_side_effects=True, vmem_limit_bytes=64 * 1024 * 1024 - 65536
        ),
        name="whole_step",
    )(
        attended,
        post_gain.reshape(1, width),
        expert_ids.T,
        gate_weights.T,
        tokens,
        input_gain.reshape(1, width),
        kv_weight,
        key_gain.reshape(1, HD),
        page_list,
        lengths,
        assignment.T,
        query,
        new_kv,
        w_gate.reshape(width, inner),
        w_up.reshape(width, inner),
        w_down.reshape(inner, width),
    )
    return pl.pallas_call(
        place_results,
        out_shape=(
            jax.ShapeDtypeStruct((rows, width), bf16),
            jax.ShapeDtypeStruct((RCAP, H * HD), bf16),
        ),
        in_specs=[pl.BlockSpec(memory_space=pltpu.HBM)] * 2,
        out_specs=(vmem, vmem),
        scratch_shapes=[pltpu.VMEM((lines, HD), f32), dma((2,))],
        compiler_params=pltpu.CompilerParams(vmem_limit_bytes=64 * 1024 * 1024 - 65536),
        name="place_results",
    )(moe_out, decode_out)


def solution(mesh):
    in_specs = (
        P(("groups", "pre", "dec"), None),
        P(("groups", "pre", "dec"), None),
        P(),
        P(),
        P("pre", None),
        P(),
        P(("pre", "dec"), None, None),
        P(("pre", "dec"), None, None),
        P(("pre", "dec"), None, None),
        P(("groups", "pre", "dec"), None),
        P(("groups", "pre", "dec"), None),
        P(("groups", "pre"), None),
        P(("groups", "pre"), None),
        P(("groups", "pre"), None),
        P(("groups", "pre"), None),
        P(("groups", "pre"), None),
    )
    out_specs = (P(("groups", "pre", "dec"), None), P(("groups", "pre", "dec"), None))
    return jax.shard_map(body, mesh=mesh, in_specs=in_specs, out_specs=out_specs, check_vma=False)
```
